32 devices in a mesh: groups: 2 (over y), range: 8 (over z, x), sub: 2 (over core).
Axes of the slice: x: 2, y: 2, z: 4, core: 2. Of those that a mesh axis runs over, the one named last changes fastest.
Arguments:
- samples: float32 [2, 1024, 32, 128], P(None, ('groups', 'range', 'sub')), parts along dimension 1, may hold values from -6 to 6
- beam_weights: float32 [32, 8, 2, 64, 128], P(('groups', 'range'), None, None, None, 'sub'), parts along dimension 0, may hold values from -0.25 to 0.25
- subarrays: int32 [32, 8, 64], P(('groups', 'range', 'sub')), parts along dimension 0, may hold values from 0 to 511, as said below
- training: int32 [64], P(('groups', 'range', 'sub')), parts along dimension 0, may hold values 0 or 1
Outputs:
- covariance: float32 [32, 8, 64, 128], P(('groups', 'range', 'sub')), parts along dimension 0
- filtered: float32 [2, 128, 64, 128], P(None, None, ('groups', 'range', 'sub')), parts along dimension 2
- energy: float32 [256], P('groups'), parts along dimension 0
The draws below stay inside these ranges and needn't reach their ends.
There are 2 independent parts, one for each index of `groups`. The reference program is written for one: setup_inputs(seed, part) draws one part's arguments, and reference() takes and returns one part's arrays. A program takes and returns all parts, laid end to end along the dimension named above; each array names one. Nothing has to cross between parts.
Inputs may be any that keep to these rules, and one draw needn't show every extreme that they name: `subarrays`: in each gate block the 512 indices are all 512 channels, each once.
All inputs are finite; a program needn't handle non-finite values. No bound on the sum of `training` on one device may be relied on, other than what follows from the above.
Results may differ from the reference program's by a relative error of at most 0.0003.
Values sent between devices are 32-bit elements; how exact they have to be, the bound alone decides.
A program may use at most 64 MiB of HBM per device.

```python
import jax
import jax.numpy as jnp
from jax import lax

C = 512
S = 64
K = 128
P_SIZE = 128
GB = 2
NS = 8
G = 32
NB = 16


def draw_subarrays(key, part):
    several = jax.random.split(jax.random.fold_in(key, 17), NB)
    orders = jax.vmap(lambda single: jax.random.permutation(single, C))(several)
    return orders.reshape(NB, NS, S).astype(jnp.int32)


def plant(values, stream_key, smallest, top_value):
    longest = values.shape.index(max(values.shape))
    spots = []
    for shift in (0, 1):
        where = [jax.random.randint(jax.random.fold_in(stream_key, axis), (), 0, length) for axis, length in enumerate(values.shape)]
        where[longest] = (where[longest] + shift) % values.shape[longest]
        spots.append(tuple(where))
    return values.at[spots[0]].set(smallest).at[spots[1]].set(top_value)


def level_of(rng, extent, cuts, least, high):
    level, own = 1.0, jax.random.fold_in(rng, 6)
    for dim, parts in cuts:
        heights = jnp.exp(jax.random.uniform(jax.random.fold_in(own, dim), (parts,), jnp.float32, least / len(cuts), high / len(cuts)))
        level = level * jnp.repeat(heights, extent[dim] // parts).reshape([-1 if axis == dim else 1 for axis in range(len(extent))])
    return level


def normal_values(key, extent, width, bound, cuts=(), kind=jnp.bfloat16):
    drawn = width * jax.random.normal(key, extent, jnp.float32)
    if cuts:
        drawn = drawn * level_of(key, extent, cuts, -0.22, 0.18)
    return jnp.clip(drawn, -bound, bound).astype(kind)


def setup_inputs(seed: int = 0, part: int = 0) -> dict:
    splits = jax.random.split(jax.random.key(seed), 5)
    part_keys = jax.random.split(jax.random.fold_in(splits[4], part), 5)
    samples = normal_values(part_keys[0], (2, C, G, P_SIZE), 1.0, 6.0, ((1, 16),), jnp.float32)
    beam_weights = normal_values(part_keys[1], (NB, NS, 2, S, K), C ** -0.5, 0.25, ((0, 8), (4, 2)), jnp.float32)
    subarrays = draw_subarrays(jax.random.fold_in(jax.random.fold_in(splits[4], part), 71), part)
    training = plant((jax.random.randint(part_keys[3], (G,), 0, 2) < 1).astype(jnp.int32), jax.random.fold_in(part_keys[3], 1), 0, 1)
    return dict(samples=samples, beam_weights=beam_weights, subarrays=subarrays, training=training)


loading = 0.05

def block_terms(snaps, chosen, weights, masked, factor):
    highest = lax.Precision.HIGHEST
    picked = jnp.take(snaps, chosen, axis=1)
    real_part = picked[0]
    imag_part = picked[1]
    real_masked = real_part * masked
    imag_masked = imag_part * masked
    cov_real = (jnp.einsum('snx,smx->snm', real_masked, real_part, precision=highest) + jnp.einsum('snx,smx->snm', imag_masked, imag_part, precision=highest)) * factor
    cov_imag = (jnp.einsum('snx,smx->snm', imag_masked, real_part, precision=highest) - jnp.einsum('snx,smx->snm', real_masked, imag_part, precision=highest)) * factor
    w_real = weights[:, 0]
    w_imag = weights[:, 1]
    out_real = jnp.einsum('snk,snx->kx', w_real, real_part, precision=highest) + jnp.einsum('snk,snx->kx', w_imag, imag_part, precision=highest)
    out_imag = jnp.einsum('snk,snx->kx', w_real, imag_part, precision=highest) - jnp.einsum('snk,snx->kx', w_imag, real_part, precision=highest)
    prod_real = jnp.einsum('snm,smk->snk', cov_real, w_real, precision=highest) - jnp.einsum('snm,smk->snk', cov_imag, w_imag, precision=highest)
    prod_imag = jnp.einsum('snm,smk->snk', cov_real, w_imag, precision=highest) + jnp.einsum('snm,smk->snk', cov_imag, w_real, precision=highest)
    quadratic = lax.optimization_barrier(jnp.sum(w_real * prod_real + w_imag * prod_imag, axis=(0, 1)))
    inverse = 1.0 / jnp.sqrt(quadratic + loading)
    filtered = jnp.stack([out_real * inverse[:, None], out_imag * inverse[:, None]])
    energy = lax.optimization_barrier(jnp.sum(out_real * out_real + out_imag * out_imag, axis=1))
    covariance = jnp.concatenate([cov_real, cov_imag], axis=-1)
    return (covariance, filtered, energy)

def reference(samples, beam_weights, subarrays, training):
    factor = 1.0 / (GB * P_SIZE)

    def one_block(index):
        start = (index * GB).astype(jnp.int32)
        snaps = lax.dynamic_slice_in_dim(samples, start, GB, 2).reshape(2, C, GB * P_SIZE)
        gates_on = lax.dynamic_slice_in_dim(training, start, GB, 0).astype(jnp.float32)
        masked = jnp.repeat(gates_on, P_SIZE)
        return block_terms(snaps, subarrays[index], beam_weights[index], masked, factor)
    covs, filts, energies = lax.map(one_block, jnp.arange(NB, dtype=jnp.int32))
    filtered = filts.reshape(NB, 2, K, GB, P_SIZE).transpose(1, 2, 0, 3, 4).reshape(2, K, G, P_SIZE)
    energy = lax.optimization_barrier(jnp.sum(energies, axis=0)) / (G * P_SIZE)
    return (covs, filtered, energy)
```

```python
import functools

import jax
import jax.numpy as jnp
from jax import lax
from jax.experimental import pallas as pl
from jax.experimental.pallas import tpu as pltpu
from jax.sharding import PartitionSpec as P

GB = 2
loading = 0.05
F32 = jnp.float32
BF16 = jnp.bfloat16
MESH = pl.DeviceIdType.MESH


def split(x):
    hi = x.astype(BF16)
    return hi, (x - hi.astype(F32)).astype(BF16)


def dot(a, b):
    return jnp.dot(a, b, preferred_element_type=F32)


def dot_t(a, b):
    return lax.dot_general(a, b, (((1,), (1,)), ((), ())), preferred_element_type=F32)


def each(count, fn, first=0):
    if count - first <= 8:
        for i in range(first, count):
            fn(i)
    else:

        def step(i, c):
            fn(i)
            return c

        lax.fori_loop(first, count, step, 0)


def kernel(
    dims,
    smp, bw, sub_in, trn_in,
    cov, filt, en,
    sub, trn, sendb, recv, wfull, sel, wl, bq, wv, eacc, gat, ev, psum, esend, erecv,
    send_sem, recv_sem, fsem, wsem, esem, lsem,
):
    n, cores, c_loc, gates, pulses, ns, s_n, k_half = dims
    beams = 2 * k_half
    chans = n * c_loc
    part, half = n // 4, n // 2
    rows = half * c_loc
    core = lax.axis_index("sub")
    me = lax.axis_index("range") * cores + core
    plane, low = me // part, me % part
    upper = plane // 2
    planes = (3 - 3 * upper, 2 - upper, plane + 1 - 2 * (plane % 2), plane)

    def where(d):
        return {"range": d // cores, "sub": d % cores}

    def device(p, i):
        return planes[p] * part + (low + i) % part

    def slots(ref, g, p, count=None):
        return ref.at[g, pl.ds(planes[p] * part, count or part)]

    def fetch(d, g, p, ref):
        return pltpu.make_async_copy(smp.at[:, d * GB + g], ref.at[g, d], fsem.at[g, p])

    def piece(d, g, p):
        return pltpu.make_async_remote_copy(
            src_ref=sendb.at[g, d],
            dst_ref=recv.at[g, me],
            send_sem=send_sem.at[0],
            recv_sem=recv_sem.at[g, p],
            device_id=where(d),
            device_id_type=MESH,
        )

    def arrived(src, dst, p, g):
        return pltpu.make_async_remote_copy(
            src_ref=src,
            dst_ref=dst,
            send_sem=send_sem.at[0],
            recv_sem=recv_sem.at[g, p],
            device_id=where(device(2, 0)),
            device_id_type=MESH,
        )

    groups = [(g, p) for g in range(GB) for p in (0, 1)] + [(g, p) for g in range(GB) for p in (2, 3)]
    for g, p in groups:
        each(part, lambda i: fetch(device(p, i), g, p, sendb).start(), int(p == 3))
    mine = [pltpu.make_async_copy(smp.at[:, me * GB + g], recv.at[g, me], lsem.at[g]) for g in range(GB)]
    keep = pltpu.make_async_copy(bw.at[core], wfull.at[core], lsem.at[2])
    small = [
        pltpu.make_async_copy(sub_in, sub, lsem.at[3]),
        pltpu.make_async_copy(trn_in, trn, lsem.at[4]),
    ]
    for copy in mine + [keep] + small:
        copy.start()

    barrier = pltpu.get_barrier_semaphore()

    def greet(p, i):
        pl.semaphore_signal(barrier, inc=1, device_id=where(device(p, i)), device_id_type=MESH)

    for p in range(4):
        each(part, functools.partial(greet, p), int(p == 3))
    pl.semaphore_wait(barrier, n - 1)

    place = (plane + upper) % 2
    for g, p in groups:
        count = part - int(p == 3)
        ref = slots(sendb, g, p, count)
        pltpu.make_async_copy(ref, ref, fsem.at[g, p]).wait()
        tag = place if p < 2 else p
        each(part, lambda i: piece(device(p, i), g, tag).start(), int(p == 3))
    swap = pltpu.make_async_remote_copy(
        src_ref=bw.at[1 - core],
        dst_ref=wfull.at[core],
        send_sem=wsem.at[0],
        recv_sem=wsem.at[1],
        device_id={"sub": 1 - core},
        device_id_type=MESH,
    )
    swap.start()

    for copy in small:
        copy.wait()
    chosen = jnp.concatenate([sub[s : s + 1, :] for s in range(ns)], axis=1)
    picks = []
    for h in range(2):
        r = lax.broadcasted_iota(jnp.int32, (rows, chans), 0)
        if c_loc % 8 == 0:
            chan = r + h * rows
        else:
            chan = (h * half + r % half) * c_loc + r // half
        pick = jnp.where(chan == chosen, 1.0, 0.0).astype(F32)
        sel[h] = jnp.transpose(pick).astype(BF16)
        picks.append(pick.astype(BF16))
    keep.wait()
    swap.wait()
    sides = []
    for iq in range(2):
        cols = []
        for s in range(ns):
            cols.append(jnp.concatenate([jnp.transpose(wfull[h, s, iq]) for h in range(2)], axis=0))
        sides.append(jnp.concatenate(cols, axis=1))
    for s in range(ns):
        w_r, w_i = (jnp.concatenate([wfull[h, s, iq] for h in range(2)], axis=1) for iq in range(2))
        both = jnp.concatenate([w_r, w_i], axis=1)
        wv[s] = both
        hi, lo = split(jnp.concatenate([both, jnp.concatenate([-w_i, w_r], axis=1)], axis=0))
        bq[s, 0] = hi
        bq[s, 1] = lo
    w_hi, w_lo = split(jnp.concatenate(sides, axis=0))
    for h in range(2):
        wl[h, 0] = dot_t(w_hi, picks[h]).astype(BF16)
        wl[h, 1] = dot_t(w_lo, picks[h]).astype(BF16)

    def build(h, g):
        sides = []
        for iq in range(2):
            j = iq * c_loc
            if c_loc % 8 == 0:
                block = recv[g, pl.ds(h * half, half), j : j + c_loc, :].reshape(rows, pulses)
            else:
                block = jnp.concatenate(
                    [
                        recv[g, pl.ds(h * half, half), j + c : j + c + 1, :].reshape(half, pulses)
                        for c in range(c_loc)
                    ],
                    axis=0,
                )
            sides.append(block)
        return split(jnp.concatenate(sides, axis=1))

    def beam(h, z_hi, z_lo):
        l_hi, l_lo = wl[h, 0], wl[h, 1]
        return dot(l_hi, z_hi) + (dot(l_hi, z_lo) + dot(l_lo, z_hi))

    def report(d):
        return pltpu.make_async_remote_copy(
            src_ref=esend,
            dst_ref=erecv.at[me],
            send_sem=esem.at[0],
            recv_sem=esem.at[1],
            device_id=where(d),
            device_id_type=MESH,
        )

    def wait_for(g, p):
        if p == 3:
            mine[g].wait()
        ref = slots(recv, g, p, part - int(p == 3))
        arrived(ref, ref, p, g).wait_recv()

    factor = 1.0 / (GB * pulses)
    for g in range(GB):
        wait_for(g, 3)
        wait_for(g, 2)
        z_hi, z_lo = build(upper, g)
        eacc[...] = beam(upper, z_hi, z_lo)
        picked = sel[upper]
        gat[0] = dot(picked, z_hi).astype(BF16)
        gat[1] = dot(picked, z_lo).astype(BF16)
        wait_for(g, 0)
        wait_for(g, 1)
        z_hi, z_lo = build(1 - upper, g)
        full = eacc[...] + beam(1 - upper, z_hi, z_lo)
        e_re = full[:beams, :pulses] + full[beams:, pulses:]
        e_im = full[:beams, pulses:] - full[beams:, :pulses]
        power = e_re * e_re + e_im * e_im
        ev[g, 0] = e_re
        ev[g, 1] = e_im
        if g < GB - 1:
            psum[...] = power if g == 0 else psum[...] + power
        else:
            p_hi, p_lo = split(psum[...] + power)
            ones = jnp.ones((8, pulses), BF16)
            esum = (dot_t(ones, p_hi) + dot_t(ones, p_lo))[0:1]
            esend[...] = esum
            erecv[me] = esum
            for j in range(3):
                other = j + (j + 4 - plane) // 4
                each(part, lambda i: report(other * part + (low + i) % part).start())
            each(part, lambda i: report(device(3, i)).start(), 1)
        picked = sel[1 - upper]
        gat[0] = (gat[0].astype(F32) + dot(picked, z_hi)).astype(BF16)
        gat[1] = (gat[1].astype(F32) + dot(picked, z_lo)).astype(BF16)
        weight = trn[g].astype(F32) * factor
        total = jnp.zeros((s_n, 2 * beams), F32)
        for s in range(ns):
            x = [gat[i, s * s_n : (s + 1) * s_n, :] for i in range(2)]
            right = [
                jnp.concatenate([v, jnp.concatenate([-v[:, pulses:], v[:, :pulses]], axis=1)], axis=0)
                for v in x
            ]
            r_s = (dot_t(x[0], right[0]) + (dot_t(x[0], right[1]) + dot_t(x[1], right[0]))) * weight
            if g > 0:
                r_s = cov[s] + r_s
            cov[s] = r_s
            if g == GB - 1:
                r_hi, r_lo = split(r_s)
                b_hi, b_lo = bq[s, 0], bq[s, 1]
                total = total + (dot(r_hi, b_hi) + (dot(r_lo, b_hi) + dot(r_hi, b_lo))) * wv[s]
    quadratic = jnp.sum(total, axis=0, keepdims=True)
    quadratic = quadratic[:, :beams] + quadratic[:, beams:]
    inverse = 1.0 / jnp.sqrt(quadratic + loading)
    scale = jnp.transpose(jnp.broadcast_to(inverse, (pulses, beams)))
    for g in range(GB):
        for iq in range(2):
            filt[iq, pl.ds(g, beams, stride=GB), :] = ev[g, iq] * scale

    sent = sendb.at[:, pl.ds(0, n - 1)]
    pltpu.make_async_remote_copy(
        src_ref=sent,
        dst_ref=sent,
        send_sem=send_sem.at[0],
        recv_sem=recv_sem.at[0, 0],
        device_id=where(device(2, 0)),
        device_id_type=MESH,
    ).wait_send()
    reports = erecv.at[pl.ds(0, n - 1)]
    shared = pltpu.make_async_remote_copy(
        src_ref=reports,
        dst_ref=reports,
        send_sem=esem.at[0],
        recv_sem=esem.at[1],
        device_id=where(device(2, 0)),
        device_id_type=MESH,
    )
    shared.wait_send()
    shared.wait_recv()
    en[...] = jnp.sum(erecv[...], axis=0) * (1.0 / (gates * pulses))


def store(cov, filt, en, cov_out, filt_out, en_out, sem):
    pairs = ((cov, cov_out), (filt, filt_out), (en, en_out))
    copies = [pltpu.make_async_copy(a, b, sem.at[i]) for i, (a, b) in enumerate(pairs)]
    for copy in copies:
        copy.start()
    for copy in copies:
        copy.wait()


def body(samples, beam_weights, subarrays, training):
    range_count = lax.axis_size("range")
    cores = lax.axis_size("sub")
    n = range_count * cores
    parts_iq, c_loc, gates, pulses = samples.shape
    blocks, ns, _, s_n, k_half = beam_weights.shape
    assert gates == GB * n and blocks == cores == 2 and subarrays.shape[0] == 1
    assert n & (n - 1) == 0 and n >= 8
    assert parts_iq == 2 and n * c_loc == ns * s_n
    beams, chans = 2 * k_half, n * c_loc
    dims = (n, cores, c_loc, gates, pulses, ns, s_n, k_half)
    hbm = pl.BlockSpec(memory_space=pl.ANY)
    vmem = pl.BlockSpec(memory_space=pltpu.VMEM)
    dma = pltpu.SemaphoreType.DMA
    cov, filt, en = pl.pallas_call(
        functools.partial(kernel, dims),
        out_shape=(
            pltpu.VMEM((ns, s_n, 2 * s_n), F32),
            pltpu.VMEM((2, beams * GB, pulses), F32),
            pltpu.VMEM((1, beams), F32),
        ),
        in_specs=[hbm] * 4,
        out_specs=(vmem, vmem, vmem),
        scratch_shapes=[
            pltpu.VMEM((ns, s_n), jnp.int32),
            pltpu.SMEM((GB,), jnp.int32),
            pltpu.VMEM((GB, n, 2 * c_loc, pulses), F32),
            pltpu.VMEM((GB, n, 2 * c_loc, pulses), F32),
            pltpu.VMEM((2, ns, 2, s_n, k_half), F32),
            pltpu.VMEM((2, chans, chans // 2), BF16),
            pltpu.VMEM((2, 2, 2 * beams, chans // 2), BF16),
            pltpu.VMEM((ns, 2, 2 * s_n, 2 * beams), BF16),
            pltpu.VMEM((ns, s_n, 2 * beams), F32),
            pltpu.VMEM((2 * beams, 2 * pulses), F32),
            pltpu.VMEM((2, chans, 2 * pulses), BF16),
            pltpu.VMEM((GB, 2, beams, pulses), F32),
            pltpu.VMEM((beams, pulses), F32),
            pltpu.VMEM((1, beams), F32),
            pltpu.VMEM((n, 1, beams), F32),
            dma((1,)),
            dma((GB, 4)),
            dma((GB, 4)),
            dma((2,)),
            dma((2,)),
            dma((5,)),
        ],
        compiler_params=pltpu.CompilerParams(collective_id=0, has_side_effects=True),
    )(
        samples.reshape(2 * c_loc, gates, pulses),
        beam_weights,
        subarrays.reshape(ns, s_n),
        training,
    )
    cov, filt, en = (pltpu.with_memory_space_constraint(v, pltpu.VMEM) for v in (cov, filt, en))
    cov, filt, en = pl.pallas_call(
        store,
        out_shape=[jax.ShapeDtypeStruct(v.shape, F32) for v in (cov, filt, en)],
        in_specs=[vmem] * 3,
        out_specs=[hbm] * 3,
        scratch_shapes=[dma((3,))],
    )(cov, filt, en)
    return (
        cov.reshape(1, ns, s_n, 2 * s_n),
        filt.reshape(2, beams, GB, pulses),
        en.reshape(beams),
    )


def solution(mesh):
    placed = (
        P(None, ("groups", "range", "sub"), None, None),
        P(("groups", "range"), None, None, None, "sub"),
        P(("groups", "range", "sub"), None, None),
        P(("groups", "range", "sub")),
    )
    return jax.shard_map(
        body,
        mesh=mesh,
        in_specs=placed,
        out_specs=(
            P(("groups", "range", "sub"), None, None, None),
            P(None, None, ("groups", "range", "sub"), None),
            P("groups"),
        ),
        check_vma=False,
    )
```

```python
import functools

import jax
import jax.numpy as jnp
from jax import lax
from jax.experimental import pallas as pl
from jax.experimental.pallas import tpu as pltpu
from jax.sharding import PartitionSpec as P

GB = 2
loading = 0.05
F32 = jnp.float32
BF16 = jnp.bfloat16
MESH = pl.DeviceIdType.MESH


def split(x):
    hi = x.astype(BF16)
    return hi, (x - hi.astype(F32)).astype(BF16)


def dot(a, b):
    return jnp.dot(a, b, preferred_element_type=F32)


def dot_t(a, b):
    return lax.dot_general(a, b, (((1,), (1,)), ((), ())), preferred_element_type=F32)


def each(count, fn, first=0):
    if count - first <= 8:
        for i in range(first, count):
            fn(i)
    else:

        def step(i, c):
            fn(i)
            return c

        lax.fori_loop(first, count, step, 0)


def kernel(
    dims,
    smp, bw, sub_in, trn_in,
    cov, filt, en,
    sub, trn, sendb, recv, wfull, sel, wl, bq, wv, eacc, gat, ev, psum, esend, erecv,
    send_sem, recv_sem, fsem, wsem, esem, lsem, near,
):
    n, cores, c_loc, gates, pulses, ns, s_n, k_half = dims
    beams = 2 * k_half
    chans = n * c_loc
    part, half = n // 4, n // 2
    rows = half * c_loc
    core = lax.axis_index("sub")
    me = lax.axis_index("range") * cores + core
    plane, low = me // part, me % part
    upper = plane // 2
    planes = (3 - 3 * upper, 2 - upper, plane + 1 - 2 * (plane % 2), plane)

    def where(d):
        return {"range": d // cores, "sub": d % cores}

    def device(p, i):
        return planes[p] * part + (low + i) % part

    def slots(ref, g, p, count=None):
        return ref.at[g, pl.ds(planes[p] * part, count or part)]

    def fetch(d, g, p, ref):
        return pltpu.make_async_copy(smp.at[:, d * GB + g], ref.at[g, d], fsem.at[g, p])

    def piece(d, g, p):
        return pltpu.make_async_remote_copy(
            src_ref=sendb.at[g, d],
            dst_ref=recv.at[g, me],
            send_sem=send_sem.at[0],
            recv_sem=recv_sem.at[g, p],
            device_id=where(d),
            device_id_type=MESH,
        )

    def arrived(src, dst, p, g):
        return pltpu.make_async_remote_copy(
            src_ref=src,
            dst_ref=dst,
            send_sem=send_sem.at[0],
            recv_sem=recv_sem.at[g, p],
            device_id=where(device(2, 0)),
            device_id_type=MESH,
        )

    groups = [(g, p) for g in range(GB) for p in (0, 1)] + [(g, p) for g in range(GB) for p in (2, 3)]
    for g, p in groups:
        each(part, lambda i: fetch(device(p, i), g, p, sendb).start(), int(p == 3))
    mine = [pltpu.make_async_copy(smp.at[:, me * GB + g], recv.at[g, me], lsem.at[g]) for g in range(GB)]
    keep = pltpu.make_async_copy(bw.at[core], wfull.at[core], lsem.at[2])
    small = [
        pltpu.make_async_copy(sub_in, sub, lsem.at[3]),
        pltpu.make_async_copy(trn_in, trn, lsem.at[4]),
    ]
    for copy in mine + [keep] + small:
        copy.start()

    barrier = pltpu.get_barrier_semaphore()
    below, above = (plane + 3) // 4, (6 - plane) // 4
    inner = below * above == 1
    place = (plane + upper) % 2
    cell = low - core

    def greet(d):
        pl.semaphore_signal(barrier, inc=1, device_id=where(d), device_id_type=MESH)

    def tell(k):
        for there, step in ((above, part), (below, -part)):

            @pl.when(there == 1)
            def _():
                pl.semaphore_signal(
                    near.at[k], inc=1, device_id=where(me + step), device_id_type=MESH
                )

    for there, step in ((below, -part), (above, part)):

        @pl.when(there == 1)
        def _():
            for j in range(cores):
                greet(me - core + step + j)

    each(part, lambda i: greet(device(3, i)), 1)

    def send(p, i, g):
        piece(device(p, i), g, place if p < 2 else p).start()

    def send_plane(p, g):
        each(part, lambda i: send(p, i, g), int(p == 3))

    def facing(j, g):
        piece(planes[1] * part + cell + j, g, place).start()

    def others(g):
        each(part - cores, lambda i: piece(planes[1] * part + (cell + cores + i) % part, g, place).start())

    for g, p in groups[: 2 * GB]:
        ref = slots(sendb, g, p)
        pltpu.make_async_copy(ref, ref, fsem.at[g, p]).wait()
    pl.semaphore_wait(barrier, part - 1 + cores * (below + above))
    tell(0)

    @pl.when(inner)
    def _():
        for g in range(GB):
            for j in range(cores):
                facing(j, g)

    pl.semaphore_wait(near.at[0], below + above)
    tell(1)

    @pl.when(inner)
    def _():
        for g in range(GB - 1):
            others(g)

    pl.semaphore_wait(near.at[1], below + above)
    tell(2)

    @pl.when(inner)
    def _():
        for g in range(GB):
            send_plane(0, g)
        others(GB - 1)

    @pl.when(jnp.logical_not(inner))
    def _():
        send_plane(1, 0)

    pl.semaphore_wait(near.at[2], below + above)

    @pl.when(jnp.logical_not(inner))
    def _():
        for g in range(GB):
            send_plane(0, g)
        for g in range(1, GB):
            send_plane(1, g)

    for g, p in groups[2 * GB :]:
        ref = slots(sendb, g, p, part - int(p == 3))
        pltpu.make_async_copy(ref, ref, fsem.at[g, p]).wait()
        send_plane(p, g)
    swap = pltpu.make_async_remote_copy(
        src_ref=bw.at[1 - core],
        dst_ref=wfull.at[core],
        send_sem=wsem.at[0],
        recv_sem=wsem.at[1],
        device_id={"sub": 1 - core},
        device_id_type=MESH,
    )
    swap.start()

    for copy in small:
        copy.wait()
    chosen = jnp.concatenate([sub[s : s + 1, :] for s in range(ns)], axis=1)
    picks = []
    for h in range(2):
        r = lax.broadcasted_iota(jnp.int32, (rows, chans), 0)
        if c_loc % 8 == 0:
            chan = r + h * rows
        else:
            chan = (h * half + r % half) * c_loc + r // half
        pick = jnp.where(chan == chosen, 1.0, 0.0).astype(F32)
        sel[h] = jnp.transpose(pick).astype(BF16)
        picks.append(pick.astype(BF16))
    keep.wait()
    swap.wait()
    sides = []
    for iq in range(2):
        cols = []
        for s in range(ns):
            cols.append(jnp.concatenate([jnp.transpose(wfull[h, s, iq]) for h in range(2)], axis=0))
        sides.append(jnp.concatenate(cols, axis=1))
    for s in range(ns):
        w_r, w_i = (jnp.concatenate([wfull[h, s, iq] for h in range(2)], axis=1) for iq in range(2))
        both = jnp.concatenate([w_r, w_i], axis=1)
        wv[s] = both
        hi, lo = split(jnp.concatenate([both, jnp.concatenate([-w_i, w_r], axis=1)], axis=0))
        bq[s, 0] = hi
        bq[s, 1] = lo
    w_hi, w_lo = split(jnp.concatenate(sides, axis=0))
    for h in range(2):
        wl[h, 0] = dot_t(w_hi, picks[h]).astype(BF16)
        wl[h, 1] = dot_t(w_lo, picks[h]).astype(BF16)

    def build(h, g):
        sides = []
        for iq in range(2):
            j = iq * c_loc
            if c_loc % 8 == 0:
                block = recv[g, pl.ds(h * half, half), j : j + c_loc, :].reshape(rows, pulses)
            else:
                block = jnp.concatenate(
                    [
                        recv[g, pl.ds(h * half, half), j + c : j + c + 1, :].reshape(half, pulses)
                        for c in range(c_loc)
                    ],
                    axis=0,
                )
            sides.append(block)
        return split(jnp.concatenate(sides, axis=1))

    def beam(h, z_hi, z_lo):
        l_hi, l_lo = wl[h, 0], wl[h, 1]
        return dot(l_hi, z_hi) + (dot(l_hi, z_lo) + dot(l_lo, z_hi))

    def report(d):
        return pltpu.make_async_remote_copy(
            src_ref=esend,
            dst_ref=erecv.at[me],
            send_sem=esem.at[0],
            recv_sem=esem.at[1],
            device_id=where(d),
            device_id_type=MESH,
        )

    def wait_for(g, p):
        if p == 3:
            mine[g].wait()
        ref = slots(recv, g, p, part - int(p == 3))
        arrived(ref, ref, p, g).wait_recv()

    factor = 1.0 / (GB * pulses)
    for g in range(GB):
        wait_for(g, 3)
        wait_for(g, 2)
        z_hi, z_lo = build(upper, g)
        eacc[...] = beam(upper, z_hi, z_lo)
        picked = sel[upper]
        gat[0] = dot(picked, z_hi).astype(BF16)
        gat[1] = dot(picked, z_lo).astype(BF16)
        wait_for(g, 0)
        wait_for(g, 1)
        z_hi, z_lo = build(1 - upper, g)
        full = eacc[...] + beam(1 - upper, z_hi, z_lo)
        e_re = full[:beams, :pulses] + full[beams:, pulses:]
        e_im = full[:beams, pulses:] - full[beams:, :pulses]
        power = e_re * e_re + e_im * e_im
        ev[g, 0] = e_re
        ev[g, 1] = e_im
        if g < GB - 1:
            psum[...] = power if g == 0 else psum[...] + power
        else:
            p_hi, p_lo = split(psum[...] + power)
            ones = jnp.ones((8, pulses), BF16)
            esum = (dot_t(ones, p_hi) + dot_t(ones, p_lo))[0:1]
            esend[...] = esum
            erecv[me] = esum
            for j in range(3):
                other = j + (j + 4 - plane) // 4
                each(part, lambda i: report(other * part + (low + i) % part).start())
            each(part, lambda i: report(device(3, i)).start(), 1)
        picked = sel[1 - upper]
        gat[0] = (gat[0].astype(F32) + dot(picked, z_hi)).astype(BF16)
        gat[1] = (gat[1].astype(F32) + dot(picked, z_lo)).astype(BF16)
        weight = trn[g].astype(F32) * factor
        total = jnp.zeros((s_n, 2 * beams), F32)
        for s in range(ns):
            x = [gat[i, s * s_n : (s + 1) * s_n, :] for i in range(2)]
            right = [
                jnp.concatenate([v, jnp.concatenate([-v[:, pulses:], v[:, :pulses]], axis=1)], axis=0)
                for v in x
            ]
            r_s = (dot_t(x[0], right[0]) + (dot_t(x[0], right[1]) + dot_t(x[1], right[0]))) * weight
            if g > 0:
                r_s = cov[s] + r_s
            cov[s] = r_s
            if g == GB - 1:
                r_hi, r_lo = split(r_s)
                b_hi, b_lo = bq[s, 0], bq[s, 1]
                total = total + (dot(r_hi, b_hi) + (dot(r_lo, b_hi) + dot(r_hi, b_lo))) * wv[s]
    quadratic = jnp.sum(total, axis=0, keepdims=True)
    quadratic = quadratic[:, :beams] + quadratic[:, beams:]
    inverse = 1.0 / jnp.sqrt(quadratic + loading)
    scale = jnp.transpose(jnp.broadcast_to(inverse, (pulses, beams)))
    for g in range(GB):
        for iq in range(2):
            filt[iq, pl.ds(g, beams, stride=GB), :] = ev[g, iq] * scale

    sent = sendb.at[:, pl.ds(0, n - 1)]
    pltpu.make_async_remote_copy(
        src_ref=sent,
        dst_ref=sent,
        send_sem=send_sem.at[0],
        recv_sem=recv_sem.at[0, 0],
        device_id=where(device(2, 0)),
        device_id_type=MESH,
    ).wait_send()
    reports = erecv.at[pl.ds(0, n - 1)]
    shared = pltpu.make_async_remote_copy(
        src_ref=reports,
        dst_ref=reports,
        send_sem=esem.at[0],
        recv_sem=esem.at[1],
        device_id=where(device(2, 0)),
        device_id_type=MESH,
    )
    shared.wait_send()
    shared.wait_recv()
    en[...] = jnp.sum(erecv[...], axis=0) * (1.0 / (gates * pulses))


def store(cov, filt, en, cov_out, filt_out, en_out, sem):
    pairs = ((cov, cov_out), (filt, filt_out), (en, en_out))
    copies = [pltpu.make_async_copy(a, b, sem.at[i]) for i, (a, b) in enumerate(pairs)]
    for copy in copies:
        copy.start()
    for copy in copies:
        copy.wait()


def body(samples, beam_weights, subarrays, training):
    range_count = lax.axis_size("range")
    cores = lax.axis_size("sub")
    n = range_count * cores
    parts_iq, c_loc, gates, pulses = samples.shape
    blocks, ns, _, s_n, k_half = beam_weights.shape
    assert gates == GB * n and blocks == cores == 2 and subarrays.shape[0] == 1
    assert n & (n - 1) == 0 and n >= 8
    assert parts_iq == 2 and n * c_loc == ns * s_n
    beams, chans = 2 * k_half, n * c_loc
    dims = (n, cores, c_loc, gates, pulses, ns, s_n, k_half)
    hbm = pl.BlockSpec(memory_space=pl.ANY)
    vmem = pl.BlockSpec(memory_space=pltpu.VMEM)
    dma = pltpu.SemaphoreType.DMA
    cov, filt, en = pl.pallas_call(
        functools.partial(kernel, dims),
        out_shape=(
            pltpu.VMEM((ns, s_n, 2 * s_n), F32),
            pltpu.VMEM((2, beams * GB, pulses), F32),
            pltpu.VMEM((1, beams), F32),
        ),
        in_specs=[hbm] * 4,
        out_specs=(vmem, vmem, vmem),
        scratch_shapes=[
            pltpu.VMEM((ns, s_n), jnp.int32),
            pltpu.SMEM((GB,), jnp.int32),
            pltpu.VMEM((GB, n, 2 * c_loc, pulses), F32),
            pltpu.VMEM((GB, n, 2 * c_loc, pulses), F32),
            pltpu.VMEM((2, ns, 2, s_n, k_half), F32),
            pltpu.VMEM((2, chans, chans // 2), BF16),
            pltpu.VMEM((2, 2, 2 * beams, chans // 2), BF16),
            pltpu.VMEM((ns, 2, 2 * s_n, 2 * beams), BF16),
            pltpu.VMEM((ns, s_n, 2 * beams), F32),
            pltpu.VMEM((2 * beams, 2 * pulses), F32),
            pltpu.VMEM((2, chans, 2 * pulses), BF16),
            pltpu.VMEM((GB, 2, beams, pulses), F32),
            pltpu.VMEM((beams, pulses), F32),
            pltpu.VMEM((1, beams), F32),
            pltpu.VMEM((n, 1, beams), F32),
            dma((1,)),
            dma((GB, 4)),
            dma((GB, 4)),
            dma((2,)),
            dma((2,)),
            dma((5,)),
            pltpu.SemaphoreType.REGULAR((3,)),
        ],
        compiler_params=pltpu.CompilerParams(collective_id=0, has_side_effects=True),
    )(
        samples.reshape(2 * c_loc, gates, pulses),
        beam_weights,
        subarrays.reshape(ns, s_n),
        training,
    )
    cov, filt, en = (pltpu.with_memory_space_constraint(v, pltpu.VMEM) for v in (cov, filt, en))
    cov, filt, en = pl.pallas_call(
        store,
        out_shape=[jax.ShapeDtypeStruct(v.shape, F32) for v in (cov, filt, en)],
        in_specs=[vmem] * 3,
        out_specs=[hbm] * 3,
        scratch_shapes=[dma((3,))],
    )(cov, filt, en)
    return (
        cov.reshape(1, ns, s_n, 2 * s_n),
        filt.reshape(2, beams, GB, pulses),
        en.reshape(beams),
    )


def solution(mesh):
    placed = (
        P(None, ("groups", "range", "sub"), None, None),
        P(("groups", "range"), None, None, None, "sub"),
        P(("groups", "range", "sub"), None, None),
        P(("groups", "range", "sub")),
    )
    return jax.shard_map(
        body,
        mesh=mesh,
        in_specs=placed,
        out_specs=(
            P(("groups", "range", "sub"), None, None, None),
            P(None, None, ("groups", "range", "sub"), None),
            P("groups"),
        ),
        check_vma=False,
    )
```

```python
import functools

import jax
import jax.numpy as jnp
from jax import lax
from jax.experimental import pallas as pl
from jax.experimental.pallas import tpu as pltpu
from jax.sharding import PartitionSpec as P

GB = 2
loading = 0.05
F32 = jnp.float32
BF16 = jnp.bfloat16
MESH = pl.DeviceIdType.MESH


def split(x):
    hi = x.astype(BF16)
    return hi, (x - hi.astype(F32)).astype(BF16)


def dot(a, b):
    return jnp.dot(a, b, preferred_element_type=F32)


def dot_t(a, b):
    return lax.dot_general(a, b, (((1,), (1,)), ((), ())), preferred_element_type=F32)


def each(count, fn, first=0):
    if count - first <= 8:
        for i in range(first, count):
            fn(i)
    else:

        def step(i, c):
            fn(i)
            return c

        lax.fori_loop(first, count, step, 0)


def kernel(
    dims,
    smp, bw, sub_in, trn_in,
    cov, filt, en,
    sub, trn, sendb, recv, wfull, sel, wl, bq, wv, eacc, gat, ev, psum, esend, erecv,
    send_sem, recv_sem, fsem, wsem, esem, lsem, near,
):
    n, cores, c_loc, gates, pulses, ns, s_n, k_half = dims
    beams = 2 * k_half
    chans = n * c_loc
    part = n // 4
    rows = part * c_loc
    core = lax.axis_index("sub")
    me = lax.axis_index("range") * cores + core
    plane, low = me // part, me % part
    upper = plane // 2
    planes = (3 - 3 * upper, 2 - upper, plane + 1 - 2 * (plane % 2), plane)

    def where(d):
        return {"range": d // cores, "sub": d % cores}

    def device(p, i):
        return planes[p] * part + (low + i) % part

    def slots(ref, g, p, count=None):
        return ref.at[g, pl.ds(planes[p] * part, count or part)]

    def fetch(d, g, p, ref):
        return pltpu.make_async_copy(smp.at[:, d * GB + g], ref.at[g, d], fsem.at[g, p])

    def piece(d, g, p):
        return pltpu.make_async_remote_copy(
            src_ref=sendb.at[g, d],
            dst_ref=recv.at[g, me],
            send_sem=send_sem.at[0],
            recv_sem=recv_sem.at[g, p],
            device_id=where(d),
            device_id_type=MESH,
        )

    def arrived(src, dst, p, g):
        return pltpu.make_async_remote_copy(
            src_ref=src,
            dst_ref=dst,
            send_sem=send_sem.at[0],
            recv_sem=recv_sem.at[g, p],
            device_id=where(device(2, 0)),
            device_id_type=MESH,
        )

    barrier = pltpu.get_barrier_semaphore()
    below, above = (plane + 3) // 4, (6 - plane) // 4

    def greet(d):
        pl.semaphore_signal(barrier, inc=1, device_id=where(d), device_id_type=MESH)

    for there, step in ((below * above, -part), (above, part)):

        @pl.when(there == 1)
        def _():
            for j in range(cores):
                greet(me - core + step + j)

    each(part, lambda i: greet(device(3, i)), 1)

    groups = [(g, p) for p in (1, 0, 2, 3) for g in range(GB)]
    for g, p in groups:
        each(part, lambda i: fetch(device(p, i), g, p, sendb).start(), int(p == 3))
    mine = [pltpu.make_async_copy(smp.at[:, me * GB + g], recv.at[g, me], lsem.at[g]) for g in range(GB)]
    keep = pltpu.make_async_copy(bw.at[core], wfull.at[core], lsem.at[2])
    small = [
        pltpu.make_async_copy(sub_in, sub, lsem.at[3]),
        pltpu.make_async_copy(trn_in, trn, lsem.at[4]),
    ]
    for copy in mine + [keep] + small:
        copy.start()

    def ready(g, p):
        ref = slots(sendb, g, p, part - int(p == 3))
        pltpu.make_async_copy(ref, ref, fsem.at[g, p]).wait()

    place = (plane + upper) % 2
    cell = low - core

    def send(p, i, g):
        piece(device(p, i), g, place if p < 2 else p).start()

    def send_plane(p, g):
        each(part, lambda i: send(p, i, g), int(p == 3))

    def facing(j, g):
        piece(planes[1] * part + cell + j, g, place).start()

    def others(g):
        each(part - cores, lambda i: piece(planes[1] * part + (cell + cores + i) % part, g, place).start())

    def tell(step, k):
        pl.semaphore_signal(near.at[k], inc=1, device_id=where(me + step), device_id_type=MESH)

    def hear(k):
        pl.semaphore_wait(near.at[k], 1)

    ready(0, 1)
    pl.semaphore_wait(barrier, part - 1 + cores * (below + above * (1 - upper)))

    @pl.when(plane == 0)
    def _():
        tell(part, 2)
        for g, p in groups[1 : 2 * GB]:
            ready(g, p)
        hear(0)
        for j in range(cores):
            facing(j, 0)
        hear(1)
        others(0)
        hear(2)
        send_plane(0, 0)
        send_plane(0, 1)
        for j in range(cores):
            each(part // cores, lambda i: piece(planes[1] * part + (cell + cores * i) % part + j, 1, place).start())

    @pl.when(plane == 1)
    def _():
        tell(part, 0)
        tell(-part, 0)
        for j in range(cores):
            facing(j, 0)
        for g, p in groups[1 : 2 * GB]:
            ready(g, p)
        hear(0)
        tell(-part, 1)
        others(0)
        hear(2)
        tell(part, 1)
        hear(1)
        tell(-part, 2)
        send_plane(0, 0)
        send_plane(0, 1)
        for j in range(cores):
            each(part // cores, lambda i: piece(planes[1] * part + (cell + cores * i) % part + j, 1, place).start())

    @pl.when(plane == 2)
    def _():
        tell(-part, 0)
        for j in range(cores):
            facing(j, 0)
        for g, p in groups[1 : 2 * GB]:
            ready(g, p)
        hear(0)
        others(0)
        hear(2)
        tell(-part, 1)
        hear(1)
        tell(part, 0)
        send_plane(0, 0)
        send_plane(0, 1)
        for j in range(cores):
            each(part // cores, lambda i: piece(planes[1] * part + (cell + cores * i) % part + j, 1, place).start())

    @pl.when(plane == 3)
    def _():
        tell(-part, 2)
        for g, p in groups[1 : 2 * GB]:
            ready(g, p)
        hear(0)
        send_plane(1, 0)
        send_plane(0, 0)
        send_plane(0, 1)
        for j in range(cores):
            each(part // cores, lambda i: piece(planes[1] * part + (cell + cores * i) % part + j, 1, place).start())

    for g, p in groups[2 * GB :]:
        ready(g, p)
        send_plane(p, g)
    swap = pltpu.make_async_remote_copy(
        src_ref=bw.at[1 - core],
        dst_ref=wfull.at[core],
        send_sem=wsem.at[0],
        recv_sem=wsem.at[1],
        device_id={"sub": 1 - core},
        device_id_type=MESH,
    )
    swap.start()

    for copy in small:
        copy.wait()
    chosen = jnp.concatenate([sub[s : s + 1, :] for s in range(ns)], axis=1)
    picks = []
    for q in range(4):
        r = lax.broadcasted_iota(jnp.int32, (rows, chans), 0)
        if c_loc % 8 == 0:
            chan = r + q * rows
        else:
            chan = (q * part + r % part) * c_loc + r // part
        pick = jnp.where(chan == chosen, 1.0, 0.0).astype(F32)
        sel[q] = jnp.transpose(pick).astype(BF16)
        picks.append(pick.astype(BF16))
    keep.wait()
    swap.wait()
    sides = []
    for iq in range(2):
        cols = []
        for s in range(ns):
            cols.append(jnp.concatenate([jnp.transpose(wfull[h, s, iq]) for h in range(2)], axis=0))
        sides.append(jnp.concatenate(cols, axis=1))
    for s in range(ns):
        w_r, w_i = (jnp.concatenate([wfull[h, s, iq] for h in range(2)], axis=1) for iq in range(2))
        both = jnp.concatenate([w_r, w_i], axis=1)
        wv[s] = both
        hi, lo = split(jnp.concatenate([both, jnp.concatenate([-w_i, w_r], axis=1)], axis=0))
        bq[s, 0] = hi
        bq[s, 1] = lo
    w_hi, w_lo = split(jnp.concatenate(sides, axis=0))
    for q in range(4):
        wl[q, 0] = dot_t(w_hi, picks[q]).astype(BF16)
        wl[q, 1] = dot_t(w_lo, picks[q]).astype(BF16)

    def build(p, g):
        q = planes[p]
        sides = []
        for iq in range(2):
            j = iq * c_loc
            if c_loc % 8 == 0:
                block = recv[g, pl.ds(q * part, part), j : j + c_loc, :].reshape(rows, pulses)
            else:
                block = jnp.concatenate(
                    [
                        recv[g, pl.ds(q * part, part), j + c : j + c + 1, :].reshape(part, pulses)
                        for c in range(c_loc)
                    ],
                    axis=0,
                )
            sides.append(block)
        return split(jnp.concatenate(sides, axis=1))

    def beam(p, z_hi, z_lo):
        l_hi, l_lo = wl[planes[p], 0], wl[planes[p], 1]
        both = dot(jnp.concatenate([l_hi, l_lo], axis=1), jnp.concatenate([z_hi, z_hi], axis=0))
        return both + dot(l_hi, z_lo)

    def gather(p, z):
        picked = sel[planes[p]]
        for i in range(2):
            gat[i] = (gat[i].astype(F32) + dot(picked, z[i])).astype(BF16)

    def report(d):
        return pltpu.make_async_remote_copy(
            src_ref=esend,
            dst_ref=erecv.at[me],
            send_sem=esem.at[0],
            recv_sem=esem.at[1],
            device_id=where(d),
            device_id_type=MESH,
        )

    def wait_for(g, p):
        if p == 3:
            mine[g].wait()
        ref = slots(recv, g, p, part - int(p == 3))
        arrived(ref, ref, p, g).wait_recv()

    factor = 1.0 / (GB * pulses)
    for g in range(GB):
        wait_for(g, 3)
        wait_for(g, 2)
        own, next_to = build(3, g), build(2, g)
        eacc[...] = beam(3, *own) + beam(2, *next_to)
        picked = jnp.concatenate([sel[planes[3]], sel[planes[2]]], axis=1)
        for i in range(2):
            gat[i] = dot(picked, jnp.concatenate([own[i], next_to[i]], axis=0)).astype(BF16)
        wait_for(g, 0)
        z = build(0, g)
        eacc[...] = eacc[...] + beam(0, *z)
        gather(0, z)
        wait_for(g, 1)
        z = build(1, g)
        full = eacc[...] + beam(1, *z)
        e_re = full[:beams, :pulses] + full[beams:, pulses:]
        e_im = full[:beams, pulses:] - full[beams:, :pulses]
        power = e_re * e_re + e_im * e_im
        if g < GB - 1:
            psum[...] = power if g == 0 else psum[...] + power
        else:
            across = jnp.transpose(psum[...] + power)
            esum = jnp.sum(across.reshape(pulses // 8, 8, beams), axis=0)
            esend[...] = esum
            erecv[me] = esum
            for j in range(3):
                other = j + (j + 4 - plane) // 4
                each(part, lambda i: report(other * part + (low + i) % part).start())
            each(part, lambda i: report(device(3, i)).start(), 1)
        ev[g, 0] = e_re
        ev[g, 1] = e_im
        gather(1, z)
        weight = trn[g].astype(F32) * factor
        for s in range(ns):
            x = [gat[i, s * s_n : (s + 1) * s_n, :] for i in range(2)]
            right = [
                jnp.concatenate([v, jnp.concatenate([-v[:, pulses:], v[:, :pulses]], axis=1)], axis=0)
                for v in x
            ]
            r_s = (dot_t(x[0], right[0]) + (dot_t(x[0], right[1]) + dot_t(x[1], right[0]))) * weight
            cov[s] = r_s if g == 0 else cov[s] + r_s
    total = jnp.zeros((8, 2 * beams), F32)
    for s in range(ns):
        r_hi, r_lo = split(cov[s])
        b_hi, b_lo = bq[s, 0], bq[s, 1]
        term = (dot(r_hi, b_hi) + (dot(r_lo, b_hi) + dot(r_hi, b_lo))) * wv[s]
        total = total + jnp.sum(term.reshape(s_n // 8, 8, 2 * beams), axis=0)
    quadratic = jnp.sum(total, axis=0, keepdims=True)
    quadratic = quadratic[:, :beams] + quadratic[:, beams:]
    inverse = 1.0 / jnp.sqrt(quadratic + loading)
    scale = jnp.transpose(jnp.broadcast_to(inverse, (pulses, beams)))
    for g in range(GB):
        for iq in range(2):
            filt[iq, pl.ds(g, beams, stride=GB), :] = ev[g, iq] * scale

    sent = sendb.at[:, pl.ds(0, n - 1)]
    pltpu.make_async_remote_copy(
        src_ref=sent,
        dst_ref=sent,
        send_sem=send_sem.at[0],
        recv_sem=recv_sem.at[0, 0],
        device_id=where(device(2, 0)),
        device_id_type=MESH,
    ).wait_send()
    reports = erecv.at[pl.ds(0, n - 1)]
    shared = pltpu.make_async_remote_copy(
        src_ref=reports,
        dst_ref=reports,
        send_sem=esem.at[0],
        recv_sem=esem.at[1],
        device_id=where(device(2, 0)),
        device_id_type=MESH,
    )
    shared.wait_send()
    shared.wait_recv()
    en[...] = jnp.sum(jnp.sum(erecv[...], axis=0), axis=0, keepdims=True) * (1.0 / (gates * pulses))


def store(cov, filt, en, cov_out, filt_out, en_out, sem):
    pairs = ((cov, cov_out), (filt, filt_out), (en, en_out))
    copies = [pltpu.make_async_copy(a, b, sem.at[i]) for i, (a, b) in enumerate(pairs)]
    for copy in copies:
        copy.start()
    for copy in copies:
        copy.wait()


def body(samples, beam_weights, subarrays, training):
    range_count = lax.axis_size("range")
    cores = lax.axis_size("sub")
    n = range_count * cores
    parts_iq, c_loc, gates, pulses = samples.shape
    blocks, ns, _, s_n, k_half = beam_weights.shape
    assert gates == GB * n and blocks == cores == 2 and subarrays.shape[0] == 1
    assert n & (n - 1) == 0 and n >= 8
    assert parts_iq == 2 and n * c_loc == ns * s_n
    beams, chans = 2 * k_half, n * c_loc
    dims = (n, cores, c_loc, gates, pulses, ns, s_n, k_half)
    hbm = pl.BlockSpec(memory_space=pl.ANY)
    vmem = pl.BlockSpec(memory_space=pltpu.VMEM)
    dma = pltpu.SemaphoreType.DMA
    cov, filt, en = pl.pallas_call(
        functools.partial(kernel, dims),
        out_shape=(
            pltpu.VMEM((ns, s_n, 2 * s_n), F32),
            pltpu.VMEM((2, beams * GB, pulses), F32),
            pltpu.VMEM((1, beams), F32),
        ),
        in_specs=[hbm] * 4,
        out_specs=(vmem, vmem, vmem),
        scratch_shapes=[
            pltpu.VMEM((ns, s_n), jnp.int32),
            pltpu.SMEM((GB,), jnp.int32),
            pltpu.VMEM((GB, n, 2 * c_loc, pulses), F32),
            pltpu.VMEM((GB, n, 2 * c_loc, pulses), F32),
            pltpu.VMEM((2, ns, 2, s_n, k_half), F32),
            pltpu.VMEM((4, chans, chans // 4), BF16),
            pltpu.VMEM((4, 2, 2 * beams, chans // 4), BF16),
            pltpu.VMEM((ns, 2, 2 * s_n, 2 * beams), BF16),
            pltpu.VMEM((ns, s_n, 2 * beams), F32),
            pltpu.VMEM((2 * beams, 2 * pulses), F32),
            pltpu.VMEM((2, chans, 2 * pulses), BF16),
            pltpu.VMEM((GB, 2, beams, pulses), F32),
            pltpu.VMEM((beams, pulses), F32),
            pltpu.VMEM((8, beams), F32),
            pltpu.VMEM((n, 8, beams), F32),
            dma((1,)),
            dma((GB, 4)),
            dma((GB, 4)),
            dma((2,)),
            dma((2,)),
            dma((5,)),
            pltpu.SemaphoreType.REGULAR((3,)),
        ],
        compiler_params=pltpu.CompilerParams(collective_id=0, has_side_effects=True),
    )(
        samples.reshape(2 * c_loc, gates, pulses),
        beam_weights,
        subarrays.reshape(ns, s_n),
        training,
    )
    cov, filt, en = (pltpu.with_memory_space_constraint(v, pltpu.VMEM) for v in (cov, filt, en))
    cov, filt, en = pl.pallas_call(
        store,
        out_shape=[jax.ShapeDtypeStruct(v.shape, F32) for v in (cov, filt, en)],
        in_specs=[vmem] * 3,
        out_specs=[hbm] * 3,
        scratch_shapes=[dma((3,))],
    )(cov, filt, en)
    return (
        cov.reshape(1, ns, s_n, 2 * s_n),
        filt.reshape(2, beams, GB, pulses),
        en.reshape(beams),
    )


def solution(mesh):
    placed = (
        P(None, ("groups", "range", "sub"), None, None),
        P(("groups", "range"), None, None, None, "sub"),
        P(("groups", "range", "sub"), None, None),
        P(("groups", "range", "sub")),
    )
    return jax.shard_map(
        body,
        mesh=mesh,
        in_specs=placed,
        out_specs=(
            P(("groups", "range", "sub"), None, None, None),
            P(None, None, ("groups", "range", "sub"), None),
            P("groups"),
        ),
        check_vma=False,
    )
```

```python
import functools

import jax
import jax.numpy as jnp
from jax import lax
from jax.experimental import pallas as pl
from jax.experimental.pallas import tpu as pltpu
from jax.sharding import PartitionSpec as P

GB = 2
loading = 0.05
F32 = jnp.float32
BF16 = jnp.bfloat16
MESH = pl.DeviceIdType.MESH


def split(x):
    hi = x.astype(BF16)
    return hi, (x - hi.astype(F32)).astype(BF16)


def dot(a, b):
    return jnp.dot(a, b, preferred_element_type=F32)


def dot_t(a, b):
    return lax.dot_general(a, b, (((1,), (1,)), ((), ())), preferred_element_type=F32)


def each(count, fn, first=0):
    if count - first <= 8:
        for i in range(first, count):
            fn(i)
    else:

        def step(i, c):
            fn(i)
            return c

        lax.fori_loop(first, count, step, 0)


def kernel(
    dims,
    smp, bw, sub_in, trn_in,
    cov, filt, en,
    sub, trn, sendb, recv, wfull, sel, wl, bq, wv, eacc, gat, ev, psum, esend, erecv,
    send_sem, recv_sem, fsem, rsem, lsem, near,
):
    n, cores, c_loc, gates, pulses, ns, s_n, k_half = dims
    beams = 2 * k_half
    chans = n * c_loc
    part = n // 4
    rows = part * c_loc
    core = lax.axis_index("sub")
    me = lax.axis_index("range") * cores + core
    plane, low = me // part, me % part
    upper = plane // 2
    planes = (3 - 3 * upper, 2 - upper, plane + 1 - 2 * (plane % 2), plane)

    def where(d):
        return {"range": d // cores, "sub": d % cores}

    def device(p, i):
        return planes[p] * part + (low + i) % part

    def slots(ref, g, p, count=None):
        return ref.at[g, pl.ds(planes[p] * part, count or part)]

    def fetch(d, g, p, ref):
        return pltpu.make_async_copy(smp.at[:, d * GB + g], ref.at[g, d], fsem.at[GB + min(p, 2) // 2 if p != 1 else g])

    def piece(d, g, p):
        return pltpu.make_async_remote_copy(
            src_ref=sendb.at[g, d],
            dst_ref=recv.at[g, me],
            send_sem=send_sem.at[0],
            recv_sem=recv_sem.at[g, min(p, 2) if isinstance(p, int) else p],
            device_id=where(d),
            device_id_type=MESH,
        )

    def arrived(src, dst, p, g):
        return pltpu.make_async_remote_copy(
            src_ref=src,
            dst_ref=dst,
            send_sem=send_sem.at[0],
            recv_sem=recv_sem.at[g, p],
            device_id=where(device(2, 0)),
            device_id_type=MESH,
        )

    barrier = pltpu.get_barrier_semaphore()
    below, above = (plane + 3) // 4, (6 - plane) // 4

    def greet(d):
        pl.semaphore_signal(barrier, inc=1, device_id=where(d), device_id_type=MESH)

    for there, step in ((below * above, -part), (above, part)):

        @pl.when(there == 1)
        def _():
            for j in range(cores):
                greet(me - core + step + j)

    each(part, lambda i: greet(device(3, i)), 1)

    groups = [(g, p) for p in (1, 0, 2, 3) for g in range(GB)]
    for g, p in groups:
        each(part, lambda i: fetch(device(p, i), g, p, sendb).start(), int(p == 3))
    mine = [pltpu.make_async_copy(smp.at[:, me * GB + g], recv.at[g, me], lsem.at[0]) for g in range(GB)]
    keep = pltpu.make_async_copy(bw.at[core], wfull.at[core], lsem.at[1])
    small = [
        pltpu.make_async_copy(sub_in, sub, lsem.at[2]),
        pltpu.make_async_copy(trn_in, trn, lsem.at[3]),
    ]
    for copy in mine + [keep] + small:
        copy.start()

    def ready(k):
        ref = (
            [slots(sendb, g, 1) for g in range(GB)]
            + [sendb.at[:, pl.ds(0, part)], sendb.at[:, pl.ds(0, 2 * part - 1)]]
        )[k]
        pltpu.make_async_copy(ref, ref, fsem.at[k]).wait()

    place = (plane + upper) % 2
    cell = low - core

    def send(p, i, g):
        piece(device(p, i), g, place if p < 2 else p).start()

    def send_plane(p, g):
        each(part, lambda i: send(p, i, g), int(p == 3))

    def facing(j, g):
        piece(planes[1] * part + cell + j, g, place).start()

    def others(g):
        each(part - cores, lambda i: piece(planes[1] * part + (cell + cores + i) % part, g, place).start())

    def tell(step, k):
        pl.semaphore_signal(near.at[k], inc=1, device_id=where(me + step), device_id_type=MESH)

    def hear(k):
        pl.semaphore_wait(near.at[k], 1)

    ready(0)
    pl.semaphore_wait(barrier, part - 1 + cores * (below + above * (1 - upper)))

    @pl.when(plane == 0)
    def _():
        tell(part, 2)
        for k in range(1, GB + 1):
            ready(k)
        hear(0)
        for j in range(cores):
            facing(j, 0)
        hear(1)
        others(0)
        hear(2)
        send_plane(0, 0)
        send_plane(0, 1)
        each(part // cores, lambda i: piece(planes[1] * part + part - cores * (i + 1), 1, place).start())
        for j in range(1, cores):
            each(part // cores, lambda i: piece(planes[1] * part + (cell + cores * (i + 1)) % part + j, 1, place).start())

    @pl.when(plane == 1)
    def _():
        tell(part, 0)
        tell(-part, 0)
        for j in range(cores):
            facing(j, 0)
        for k in range(1, GB + 1):
            ready(k)
        hear(0)
        tell(-part, 1)
        others(0)
        hear(2)
        tell(part, 1)
        hear(1)
        tell(-part, 2)
        send_plane(0, 0)
        send_plane(0, 1)
        each(part // cores, lambda i: piece(planes[1] * part + part - cores * (i + 1), 1, place).start())
        for j in range(1, cores):
            each(part // cores, lambda i: piece(planes[1] * part + (cell + cores * (i + 1)) % part + j, 1, place).start())

    @pl.when(plane == 2)
    def _():
        tell(-part, 0)
        for j in range(cores):
            facing(j, 0)
        for k in range(1, GB + 1):
            ready(k)
        hear(0)
        others(0)
        hear(2)
        tell(-part, 1)
        hear(1)
        tell(part, 0)
        send_plane(0, 0)
        each(part - cores, lambda i: piece(planes[0] * part + cores + (low + i) % (part - cores), 1, place).start())
        for j in range(cores):
            each(part // cores, lambda i: piece(planes[1] * part + (cell + cores * i) % part + j, 1, place).start())
        each(cores, lambda i: piece(planes[0] * part + i, 1, place).start())

    @pl.when(plane == 3)
    def _():
        tell(-part, 2)
        for k in range(1, GB + 1):
            ready(k)
        hear(0)
        send_plane(1, 0)
        send_plane(0, 0)
        each(part - cores, lambda i: piece(planes[0] * part + cores + (low + i) % (part - cores), 1, place).start())
        for j in range(cores):
            each(part // cores, lambda i: piece(planes[1] * part + (cell + cores * i) % part + j, 1, place).start())
        each(cores, lambda i: piece(planes[0] * part + i, 1, place).start())

    ready(GB + 1)
    for g, p in groups[2 * GB :]:
        send_plane(p, g)
    for copy in small:
        copy.wait()
    swap = pltpu.make_async_remote_copy(
        src_ref=bw.at[1 - core],
        dst_ref=wfull.at[core],
        send_sem=lsem.at[2],
        recv_sem=rsem.at[0],
        device_id={"sub": 1 - core},
        device_id_type=MESH,
    )
    swap.start()

    chosen = jnp.concatenate([sub[s : s + 1, :] for s in range(ns)], axis=1)
    picks = []
    for q in range(4):
        r = lax.broadcasted_iota(jnp.int32, (rows, chans), 0)
        if c_loc % 8 == 0:
            chan = r + q * rows
        else:
            chan = (q * part + r % part) * c_loc + r // part
        pick = jnp.where(chan == chosen, 1.0, 0.0).astype(F32)
        sel[q] = jnp.transpose(pick).astype(BF16)
        picks.append(pick.astype(BF16))
    keep.wait()
    swap.wait()
    sides = []
    for iq in range(2):
        cols = []
        for s in range(ns):
            cols.append(jnp.concatenate([jnp.transpose(wfull[h, s, iq]) for h in range(2)], axis=0))
        sides.append(jnp.concatenate(cols, axis=1))
    for s in range(ns):
        w_r, w_i = (jnp.concatenate([wfull[h, s, iq] for h in range(2)], axis=1) for iq in range(2))
        both = jnp.concatenate([w_r, w_i], axis=1)
        wv[s] = both
        hi, lo = split(jnp.concatenate([both, jnp.concatenate([-w_i, w_r], axis=1)], axis=0))
        bq[s, 0] = hi
        bq[s, 1] = lo
    w_hi, w_lo = split(jnp.concatenate(sides, axis=0))
    for q in range(4):
        wl[q, 0] = dot_t(w_hi, picks[q]).astype(BF16)
        wl[q, 1] = dot_t(w_lo, picks[q]).astype(BF16)

    def build(p, g):
        q = planes[p]
        sides = []
        for iq in range(2):
            j = iq * c_loc
            if c_loc % 8 == 0:
                block = recv[g, pl.ds(q * part, part), j : j + c_loc, :].reshape(rows, pulses)
            else:
                block = jnp.concatenate(
                    [
                        recv[g, pl.ds(q * part, part), j + c : j + c + 1, :].reshape(part, pulses)
                        for c in range(c_loc)
                    ],
                    axis=0,
                )
            sides.append(block)
        return split(jnp.concatenate(sides, axis=1))

    def beam(p, z_hi, z_lo):
        l_hi, l_lo = wl[planes[p], 0], wl[planes[p], 1]
        both = dot(jnp.concatenate([l_hi, l_lo], axis=1), jnp.concatenate([z_hi, z_hi], axis=0))
        return both + dot(l_hi, z_lo)

    def gather(p, z):
        picked = sel[planes[p]]
        for i in range(2):
            gat[i] = (gat[i].astype(F32) + dot(picked, z[i])).astype(BF16)

    def report(d):
        return pltpu.make_async_remote_copy(
            src_ref=esend,
            dst_ref=erecv.at[me],
            send_sem=lsem.at[3],
            recv_sem=rsem.at[1],
            device_id=where(d),
            device_id_type=MESH,
        )

    def wait_for(g, p):
        if p == 2 and g == 0:
            pltpu.make_async_copy(recv.at[:, me], recv.at[:, me], lsem.at[0]).wait()
        ref = recv.at[g, pl.ds(0, 2 * part - 1)] if p == 2 else slots(recv, g, p)
        arrived(ref, ref, p, g).wait_recv()

    factor = 1.0 / (GB * pulses)
    for g in range(GB):
        wait_for(g, 2)
        own, next_to = build(3, g), build(2, g)
        eacc[...] = beam(3, *own) + beam(2, *next_to)
        picked = jnp.concatenate([sel[planes[3]], sel[planes[2]]], axis=1)
        for i in range(2):
            gat[i] = dot(picked, jnp.concatenate([own[i], next_to[i]], axis=0)).astype(BF16)
        wait_for(g, 0)
        z = build(0, g)
        eacc[...] = eacc[...] + beam(0, *z)
        gather(0, z)
        wait_for(g, 1)
        z = build(1, g)
        full = eacc[...] + beam(1, *z)
        e_re = full[:beams, :pulses] + full[beams:, pulses:]
        e_im = full[:beams, pulses:] - full[beams:, :pulses]
        power = e_re * e_re + e_im * e_im
        if g < GB - 1:
            psum[...] = power if g == 0 else psum[...] + power
        else:
            across = jnp.transpose(psum[...] + power)
            esum = jnp.sum(across.reshape(pulses // 8, 8, beams), axis=0)
            esend[...] = esum
            erecv[me] = esum
            for j in range(3):
                other = j + (j + 4 - plane) // 4
                each(part, lambda i: report(other * part + (low + i) % part).start())
            each(part, lambda i: report(device(3, i)).start(), 1)
        ev[g, 0] = e_re
        ev[g, 1] = e_im
        gather(1, z)
        weight = trn[g].astype(F32) * factor
        for s in range(ns):
            x = [gat[i, s * s_n : (s + 1) * s_n, :] for i in range(2)]
            right = [
                jnp.concatenate([v, jnp.concatenate([-v[:, pulses:], v[:, :pulses]], axis=1)], axis=0)
                for v in x
            ]
            r_s = (dot_t(x[0], right[0]) + (dot_t(x[0], right[1]) + dot_t(x[1], right[0]))) * weight
            cov[s] = r_s if g == 0 else cov[s] + r_s
    total = jnp.zeros((8, 2 * beams), F32)
    for s in range(ns):
        r_hi, r_lo = split(cov[s])
        b_hi, b_lo = bq[s, 0], bq[s, 1]
        term = (dot(r_hi, b_hi) + (dot(r_lo, b_hi) + dot(r_hi, b_lo))) * wv[s]
        total = total + jnp.sum(term.reshape(s_n // 8, 8, 2 * beams), axis=0)
    quadratic = jnp.sum(total, axis=0, keepdims=True)
    quadratic = quadratic[:, :beams] + quadratic[:, beams:]
    inverse = 1.0 / jnp.sqrt(quadratic + loading)
    scale = jnp.transpose(jnp.broadcast_to(inverse, (pulses, beams)))
    for g in range(GB):
        for iq in range(2):
            filt[iq, pl.ds(g, beams, stride=GB), :] = ev[g, iq] * scale

    sent = sendb.at[:, pl.ds(0, n - 1)]
    pltpu.make_async_remote_copy(
        src_ref=sent,
        dst_ref=sent,
        send_sem=send_sem.at[0],
        recv_sem=recv_sem.at[0, 0],
        device_id=where(device(2, 0)),
        device_id_type=MESH,
    ).wait_send()
    reports = erecv.at[pl.ds(0, n - 1)]
    shared = pltpu.make_async_remote_copy(
        src_ref=reports,
        dst_ref=reports,
        send_sem=lsem.at[3],
        recv_sem=rsem.at[1],
        device_id=where(device(2, 0)),
        device_id_type=MESH,
    )
    shared.wait_send()
    shared.wait_recv()
    en[...] = jnp.sum(jnp.sum(erecv[...], axis=0), axis=0, keepdims=True) * (1.0 / (gates * pulses))


def store(cov, filt, en, cov_out, filt_out, en_out, sem):
    pairs = ((cov, cov_out), (filt, filt_out), (en, en_out))
    copies = [pltpu.make_async_copy(a, b, sem.at[i]) for i, (a, b) in enumerate(pairs)]
    for copy in copies:
        copy.start()
    for copy in copies:
        copy.wait()


def body(samples, beam_weights, subarrays, training):
    range_count = lax.axis_size("range")
    cores = lax.axis_size("sub")
    n = range_count * cores
    parts_iq, c_loc, gates, pulses = samples.shape
    blocks, ns, _, s_n, k_half = beam_weights.shape
    assert gates == GB * n and blocks == cores == 2 and subarrays.shape[0] == 1
    assert n & (n - 1) == 0 and n >= 8
    assert parts_iq == 2 and n * c_loc == ns * s_n
    beams, chans = 2 * k_half, n * c_loc
    dims = (n, cores, c_loc, gates, pulses, ns, s_n, k_half)
    hbm = pl.BlockSpec(memory_space=pl.ANY)
    vmem = pl.BlockSpec(memory_space=pltpu.VMEM)
    dma = pltpu.SemaphoreType.DMA
    cov, filt, en = pl.pallas_call(
        functools.partial(kernel, dims),
        out_shape=(
            pltpu.VMEM((ns, s_n, 2 * s_n), F32),
            pltpu.VMEM((2, beams * GB, pulses), F32),
            pltpu.VMEM((1, beams), F32),
        ),
        in_specs=[hbm] * 4,
        out_specs=(vmem, vmem, vmem),
        scratch_shapes=[
            pltpu.VMEM((ns, s_n), jnp.int32),
            pltpu.SMEM((GB,), jnp.int32),
            pltpu.VMEM((GB, n, 2 * c_loc, pulses), F32),
            pltpu.VMEM((GB, n, 2 * c_loc, pulses), F32),
            pltpu.VMEM((2, ns, 2, s_n, k_half), F32),
            pltpu.VMEM((4, chans, chans // 4), BF16),
            pltpu.VMEM((4, 2, 2 * beams, chans // 4), BF16),
            pltpu.VMEM((ns, 2, 2 * s_n, 2 * beams), BF16),
            pltpu.VMEM((ns, s_n, 2 * beams), F32),
            pltpu.VMEM((2 * beams, 2 * pulses), F32),
            pltpu.VMEM((2, chans, 2 * pulses), BF16),
            pltpu.VMEM((GB, 2, beams, pulses), F32),
            pltpu.VMEM((beams, pulses), F32),
            pltpu.VMEM((8, beams), F32),
            pltpu.VMEM((n, 8, beams), F32),
            dma((1,)),
            dma((GB, 3)),
            dma((GB + 2,)),
            dma((2,)),
            dma((4,)),
            pltpu.SemaphoreType.REGULAR((3,)),
        ],
        compiler_params=pltpu.CompilerParams(collective_id=0, has_side_effects=True),
    )(
        samples.reshape(2 * c_loc, gates, pulses),
        beam_weights,
        subarrays.reshape(ns, s_n),
        training,
    )
    cov, filt, en = (pltpu.with_memory_space_constraint(v, pltpu.VMEM) for v in (cov, filt, en))
    cov, filt, en = pl.pallas_call(
        store,
        out_shape=[jax.ShapeDtypeStruct(v.shape, F32) for v in (cov, filt, en)],
        in_specs=[vmem] * 3,
        out_specs=[hbm] * 3,
        scratch_shapes=[dma((3,))],
    )(cov, filt, en)
    return (
        cov.reshape(1, ns, s_n, 2 * s_n),
        filt.reshape(2, beams, GB, pulses),
        en.reshape(beams),
    )


def solution(mesh):
    placed = (
        P(None, ("groups", "range", "sub"), None, None),
        P(("groups", "range"), None, None, None, "sub"),
        P(("groups", "range", "sub"), None, None),
        P(("groups", "range", "sub")),
    )
    return jax.shard_map(
        body,
        mesh=mesh,
        in_specs=placed,
        out_specs=(
            P(("groups", "range", "sub"), None, None, None),
            P(None, None, ("groups", "range", "sub"), None),
            P("groups"),
        ),
        check_vma=False,
    )
```

```python
import functools

import jax
import jax.numpy as jnp
from jax import lax
from jax.experimental import pallas as pl
from jax.experimental.pallas import tpu as pltpu
from jax.sharding import PartitionSpec as P

GB = 2
loading = 0.05
F32 = jnp.float32
BF16 = jnp.bfloat16
MESH = pl.DeviceIdType.MESH


def split(x):
    hi = x.astype(BF16)
    return hi, (x - hi.astype(F32)).astype(BF16)


def dot(a, b):
    return jnp.dot(a, b, preferred_element_type=F32)


def dot_t(a, b):
    return lax.dot_general(a, b, (((1,), (1,)), ((), ())), preferred_element_type=F32)


def each(count, fn, first=0):
    if count - first <= 8:
        for i in range(first, count):
            fn(i)
    else:

        def step(i, c):
            fn(i)
            return c

        lax.fori_loop(first, count, step, 0)


def kernel(
    dims,
    smp, bw, sub_in, trn_in,
    cov, filt, en,
    sub, trn, sendb, recv, wfull, sel, wl, bq, wv, eacc, gat, ev, psum, esend, erecv,
    send_sem, recv_sem, fsem, rsem, lsem, near,
):
    n, cores, c_loc, gates, pulses, ns, s_n, k_half = dims
    beams = 2 * k_half
    chans = n * c_loc
    part = n // 4
    rows = part * c_loc
    core = lax.axis_index("sub")
    me = lax.axis_index("range") * cores + core
    plane, low = me // part, me % part
    upper = plane // 2
    planes = (3 - 3 * upper, 2 - upper, plane + 1 - 2 * (plane % 2), plane)

    def where(d):
        return {"range": d // cores, "sub": d % cores}

    def device(p, i):
        return planes[p] * part + (low + i) % part

    def slots(ref, g, p, count=None):
        return ref.at[g, pl.ds(planes[p] * part, count or part)]

    def fetch(d, g, p, ref):
        return pltpu.make_async_copy(smp.at[:, d * GB + g], ref.at[g, d], fsem.at[GB + min(p, 2) // 2 if p != 1 else g])

    def piece(d, g, p):
        return pltpu.make_async_remote_copy(
            src_ref=sendb.at[g, d],
            dst_ref=recv.at[g, me],
            send_sem=send_sem.at[0],
            recv_sem=recv_sem.at[g, min(p, 2) if isinstance(p, int) else p],
            device_id=where(d),
            device_id_type=MESH,
        )

    def arrived(src, dst, p, g):
        return pltpu.make_async_remote_copy(
            src_ref=src,
            dst_ref=dst,
            send_sem=send_sem.at[0],
            recv_sem=recv_sem.at[g, p],
            device_id=where(device(2, 0)),
            device_id_type=MESH,
        )

    barrier = pltpu.get_barrier_semaphore()
    below, above = (plane + 3) // 4, (6 - plane) // 4

    def greet(d):
        pl.semaphore_signal(barrier, inc=1, device_id=where(d), device_id_type=MESH)

    for there, step in ((below * above, -part), (above, part)):

        @pl.when(there == 1)
        def _():
            for j in range(cores):
                greet(me - core + step + j)

    each(part, lambda i: greet(device(3, i)), 1)

    groups = [(g, p) for p in (1, 0, 2, 3) for g in range(GB)]
    for g, p in groups:
        each(part, lambda i: fetch(device(p, i), g, p, sendb).start(), int(p == 3))
    mine = [pltpu.make_async_copy(smp.at[:, me * GB + g], recv.at[g, me], lsem.at[0]) for g in range(GB)]
    keep = pltpu.make_async_copy(bw.at[core], wfull.at[core], lsem.at[1])
    small = [
        pltpu.make_async_copy(sub_in, sub, lsem.at[2]),
        pltpu.make_async_copy(trn_in, trn, lsem.at[3]),
    ]
    for copy in mine + [keep] + small:
        copy.start()

    def ready(k):
        ref = (
            [slots(sendb, g, 1) for g in range(GB)]
            + [sendb.at[:, pl.ds(0, part)], sendb.at[:, pl.ds(0, 2 * part - 1)]]
        )[k]
        pltpu.make_async_copy(ref, ref, fsem.at[k]).wait()

    place = (plane + upper) % 2
    cell = low - core

    def send(p, i, g):
        piece(device(p, i), g, place if p < 2 else p).start()

    def send_plane(p, g):
        each(part, lambda i: send(p, i, g), int(p == 3))

    def facing(j, g):
        piece(planes[1] * part + cell + j, g, place).start()

    def others(g):
        each(part - cores, lambda i: piece(planes[1] * part + (cell + cores + i) % part, g, place).start())

    def tell(step, k):
        pl.semaphore_signal(near.at[k], inc=1, device_id=where(me + step), device_id_type=MESH)

    def hear(k):
        pl.semaphore_wait(near.at[k], 1)

    ready(0)
    pl.semaphore_wait(barrier, part - 1 + cores * (below + above * (1 - upper)))

    @pl.when(plane == 0)
    def _():
        tell(part, 2)
        for k in range(1, GB + 1):
            ready(k)
        hear(0)
        for j in range(cores):
            facing(j, 0)
        hear(1)
        others(0)
        hear(2)
        send_plane(0, 1)
        send_plane(0, 0)
        each(part // cores, lambda i: piece(planes[1] * part + part - cores * (i + 1), 1, place).start())
        for j in range(1, cores):
            each(part // cores, lambda i: piece(planes[1] * part + (cell + cores * (i + 1)) % part + j, 1, place).start())

    @pl.when(plane == 1)
    def _():
        tell(part, 0)
        tell(-part, 0)
        for j in range(cores):
            facing(j, 0)
        for k in range(1, GB + 1):
            ready(k)
        hear(0)
        tell(-part, 1)
        others(0)
        hear(2)
        tell(part, 1)
        hear(1)
        tell(-part, 2)
        send_plane(0, 0)
        send_plane(0, 1)
        each(part // cores, lambda i: piece(planes[1] * part + part - cores * (i + 1), 1, place).start())
        for j in range(1, cores):
            each(part // cores, lambda i: piece(planes[1] * part + (cell + cores * (i + 1)) % part + j, 1, place).start())

    @pl.when(plane == 2)
    def _():
        tell(-part, 0)
        for j in range(cores):
            facing(j, 0)
        for k in range(1, GB + 1):
            ready(k)
        hear(0)
        others(0)
        hear(2)
        tell(-part, 1)
        hear(1)
        tell(part, 0)
        send_plane(0, 0)
        each(part - cores, lambda i: piece(planes[0] * part + cores + (low + i) % (part - cores), 1, place).start())
        for j in range(cores):
            each(part // cores, lambda i: piece(planes[1] * part + (cell + cores * i) % part + j, 1, place).start())
        each(cores, lambda i: piece(planes[0] * part + i, 1, place).start())

    @pl.when(plane == 3)
    def _():
        tell(-part, 2)
        for k in range(1, GB + 1):
            ready(k)
        hear(0)
        send_plane(1, 0)
        send_plane(0, 0)
        each(part - cores, lambda i: piece(planes[0] * part + cores + (low + i) % (part - cores), 1, place).start())
        each(cores, lambda i: piece(planes[0] * part + i, 1, place).start())
        for j in range(cores):
            each(part // cores, lambda i: piece(planes[1] * part + (cell + cores * i) % part + j, 1, place).start())

    ready(GB + 1)
    for g, p in groups[2 * GB :]:
        send_plane(p, g)
    for copy in small:
        copy.wait()
    swap = pltpu.make_async_remote_copy(
        src_ref=bw.at[1 - core],
        dst_ref=wfull.at[core],
        send_sem=lsem.at[2],
        recv_sem=rsem.at[0],
        device_id={"sub": 1 - core},
        device_id_type=MESH,
    )
    swap.start()

    chosen = jnp.concatenate([sub[s : s + 1, :] for s in range(ns)], axis=1)
    picks = []
    for q in range(4):
        r = lax.broadcasted_iota(jnp.int32, (rows, chans), 0)
        if c_loc % 8 == 0:
            chan = r + q * rows
        else:
            chan = (q * part + r % part) * c_loc + r // part
        pick = jnp.where(chan == chosen, 1.0, 0.0).astype(F32)
        sel[q] = jnp.transpose(pick).astype(BF16)
        picks.append(pick.astype(BF16))
    keep.wait()
    swap.wait()
    sides = []
    for iq in range(2):
        cols = []
        for s in range(ns):
            cols.append(jnp.concatenate([jnp.transpose(wfull[h, s, iq]) for h in range(2)], axis=0))
        sides.append(jnp.concatenate(cols, axis=1))
    for s in range(ns):
        w_r, w_i = (jnp.concatenate([wfull[h, s, iq] for h in range(2)], axis=1) for iq in range(2))
        both = jnp.concatenate([w_r, w_i], axis=1)
        wv[s] = both
        hi, lo = split(jnp.concatenate([both, jnp.concatenate([-w_i, w_r], axis=1)], axis=0))
        bq[s, 0] = hi
        bq[s, 1] = lo
    w_hi, w_lo = split(jnp.concatenate(sides, axis=0))
    for q in range(4):
        wl[q, 0] = dot_t(w_hi, picks[q]).astype(BF16)
        wl[q, 1] = dot_t(w_lo, picks[q]).astype(BF16)

    def build(p, g):
        q = planes[p]
        sides = []
        for iq in range(2):
            j = iq * c_loc
            if c_loc % 8 == 0:
                block = recv[g, pl.ds(q * part, part), j : j + c_loc, :].reshape(rows, pulses)
            else:
                block = jnp.concatenate(
                    [
                        recv[g, pl.ds(q * part, part), j + c : j + c + 1, :].reshape(part, pulses)
                        for c in range(c_loc)
                    ],
                    axis=0,
                )
            sides.append(block)
        return split(jnp.concatenate(sides, axis=1))

    def beam(p, z_hi, z_lo):
        l_hi, l_lo = wl[planes[p], 0], wl[planes[p], 1]
        both = dot(jnp.concatenate([l_hi, l_lo], axis=1), jnp.concatenate([z_hi, z_hi], axis=0))
        return both + dot(l_hi, z_lo)

    def gather(p, z):
        picked = sel[planes[p]]
        for i in range(2):
            gat[i] = (gat[i].astype(F32) + dot(picked, z[i])).astype(BF16)

    def report(d):
        return pltpu.make_async_remote_copy(
            src_ref=esend,
            dst_ref=erecv.at[me],
            send_sem=lsem.at[3],
            recv_sem=rsem.at[1],
            device_id=where(d),
            device_id_type=MESH,
        )

    def wait_for(g, p):
        if p == 2 and g == 0:
            pltpu.make_async_copy(recv.at[:, me], recv.at[:, me], lsem.at[0]).wait()
        ref = recv.at[g, pl.ds(0, 2 * part - 1)] if p == 2 else slots(recv, g, p)
        arrived(ref, ref, p, g).wait_recv()

    factor = 1.0 / (GB * pulses)
    for g in range(GB):
        wait_for(g, 2)
        own, next_to = build(3, g), build(2, g)
        eacc[...] = beam(3, *own) + beam(2, *next_to)
        picked = jnp.concatenate([sel[planes[3]], sel[planes[2]]], axis=1)
        for i in range(2):
            gat[i] = dot(picked, jnp.concatenate([own[i], next_to[i]], axis=0)).astype(BF16)
        wait_for(g, 0)
        z = build(0, g)
        eacc[...] = eacc[...] + beam(0, *z)
        gather(0, z)
        wait_for(g, 1)
        z = build(1, g)
        full = eacc[...] + beam(1, *z)
        e_re = full[:beams, :pulses] + full[beams:, pulses:]
        e_im = full[:beams, pulses:] - full[beams:, :pulses]
        power = e_re * e_re + e_im * e_im
        if g < GB - 1:
            folded = jnp.sum(jnp.transpose(power).reshape(pulses // 8, 8, beams), axis=0)
            psum[...] = folded if g == 0 else psum[...] + folded
        else:
            across = jnp.transpose(power)
            esum = psum[...] + jnp.sum(across.reshape(pulses // 8, 8, beams), axis=0)
            esend[...] = esum
            erecv[me] = esum
            for j in range(3):
                other = j + (j + 4 - plane) // 4
                each(part, lambda i: report(other * part + (low + i) % part).start())
            each(part, lambda i: report(device(3, i)).start(), 1)
        ev[g, 0] = e_re
        ev[g, 1] = e_im
        gather(1, z)
        weight = trn[g].astype(F32) * factor
        for s in range(ns):
            x = [gat[i, s * s_n : (s + 1) * s_n, :] for i in range(2)]
            right = [
                jnp.concatenate([v, jnp.concatenate([-v[:, pulses:], v[:, :pulses]], axis=1)], axis=0)
                for v in x
            ]
            r_s = (dot_t(x[0], right[0]) + (dot_t(x[0], right[1]) + dot_t(x[1], right[0]))) * weight
            cov[s] = r_s if g == 0 else cov[s] + r_s
    total = jnp.zeros((8, 2 * beams), F32)
    for s in range(ns):
        r_hi, r_lo = split(cov[s])
        b_hi, b_lo = bq[s, 0], bq[s, 1]
        term = (dot(r_hi, b_hi) + (dot(r_lo, b_hi) + dot(r_hi, b_lo))) * wv[s]
        total = total + jnp.sum(term.reshape(s_n // 8, 8, 2 * beams), axis=0)
    quadratic = jnp.sum(total, axis=0, keepdims=True)
    quadratic = quadratic[:, :beams] + quadratic[:, beams:]
    inverse = 1.0 / jnp.sqrt(quadratic + loading)
    scale = jnp.transpose(jnp.broadcast_to(inverse, (pulses, beams)))
    for g in range(GB):
        for iq in range(2):
            filt[iq, pl.ds(g, beams, stride=GB), :] = ev[g, iq] * scale

    sent = sendb.at[:, pl.ds(0, n - 1)]
    pltpu.make_async_remote_copy(
        src_ref=sent,
        dst_ref=sent,
        send_sem=send_sem.at[0],
        recv_sem=recv_sem.at[0, 0],
        device_id=where(device(2, 0)),
        device_id_type=MESH,
    ).wait_send()
    reports = erecv.at[pl.ds(0, n - 1)]
    shared = pltpu.make_async_remote_copy(
        src_ref=reports,
        dst_ref=reports,
        send_sem=lsem.at[3],
        recv_sem=rsem.at[1],
        device_id=where(device(2, 0)),
        device_id_type=MESH,
    )
    shared.wait_send()
    shared.wait_recv()
    en[...] = jnp.sum(jnp.sum(erecv[...], axis=0), axis=0, keepdims=True) * (1.0 / (gates * pulses))


def store(cov, filt, en, cov_out, filt_out, en_out, sem):
    pairs = ((en, en_out), (filt, filt_out), (cov, cov_out))
    copies = [pltpu.make_async_copy(a, b, sem.at[i]) for i, (a, b) in enumerate(pairs)]
    for copy in copies:
        copy.start()
    for copy in copies:
        copy.wait()


def body(samples, beam_weights, subarrays, training):
    range_count = lax.axis_size("range")
    cores = lax.axis_size("sub")
    n = range_count * cores
    parts_iq, c_loc, gates, pulses = samples.shape
    blocks, ns, _, s_n, k_half = beam_weights.shape
    assert gates == GB * n and blocks == cores == 2 and subarrays.shape[0] == 1
    assert n & (n - 1) == 0 and n >= 8
    assert parts_iq == 2 and n * c_loc == ns * s_n
    beams, chans = 2 * k_half, n * c_loc
    dims = (n, cores, c_loc, gates, pulses, ns, s_n, k_half)
    hbm = pl.BlockSpec(memory_space=pl.ANY)
    vmem = pl.BlockSpec(memory_space=pltpu.VMEM)
    dma = pltpu.SemaphoreType.DMA
    cov, filt, en = pl.pallas_call(
        functools.partial(kernel, dims),
        out_shape=(
            pltpu.VMEM((ns, s_n, 2 * s_n), F32),
            pltpu.VMEM((2, beams * GB, pulses), F32),
            pltpu.VMEM((1, beams), F32),
        ),
        in_specs=[hbm] * 4,
        out_specs=(vmem, vmem, vmem),
        scratch_shapes=[
            pltpu.VMEM((ns, s_n), jnp.int32),
            pltpu.SMEM((GB,), jnp.int32),
            pltpu.VMEM((GB, n, 2 * c_loc, pulses), F32),
            pltpu.VMEM((GB, n, 2 * c_loc, pulses), F32),
            pltpu.VMEM((2, ns, 2, s_n, k_half), F32),
            pltpu.VMEM((4, chans, chans // 4), BF16),
            pltpu.VMEM((4, 2, 2 * beams, chans // 4), BF16),
            pltpu.VMEM((ns, 2, 2 * s_n, 2 * beams), BF16),
            pltpu.VMEM((ns, s_n, 2 * beams), F32),
            pltpu.VMEM((2 * beams, 2 * pulses), F32),
            pltpu.VMEM((2, chans, 2 * pulses), BF16),
            pltpu.VMEM((GB, 2, beams, pulses), F32),
            pltpu.VMEM((8, beams), F32),
            pltpu.VMEM((8, beams), F32),
            pltpu.VMEM((n, 8, beams), F32),
            dma((1,)),
            dma((GB, 3)),
            dma((GB + 2,)),
            dma((2,)),
            dma((4,)),
            pltpu.SemaphoreType.REGULAR((3,)),
        ],
        compiler_params=pltpu.CompilerParams(collective_id=0, has_side_effects=True),
    )(
        samples.reshape(2 * c_loc, gates, pulses),
        beam_weights,
        subarrays.reshape(ns, s_n),
        training,
    )
    cov, filt, en = (pltpu.with_memory_space_constraint(v, pltpu.VMEM) for v in (cov, filt, en))
    cov, filt, en = pl.pallas_call(
        store,
        out_shape=[jax.ShapeDtypeStruct(v.shape, F32) for v in (cov, filt, en)],
        in_specs=[vmem] * 3,
        out_specs=[hbm] * 3,
        scratch_shapes=[dma((3,))],
    )(cov, filt, en)
    return (
        cov.reshape(1, ns, s_n, 2 * s_n),
        filt.reshape(2, beams, GB, pulses),
        en.reshape(beams),
    )


def solution(mesh):
    placed = (
        P(None, ("groups", "range", "sub"), None, None),
        P(("groups", "range"), None, None, None, "sub"),
        P(("groups", "range", "sub"), None, None),
        P(("groups", "range", "sub")),
    )
    return jax.shard_map(
        body,
        mesh=mesh,
        in_specs=placed,
        out_specs=(
            P(("groups", "range", "sub"), None, None, None),
            P(None, None, ("groups", "range", "sub"), None),
            P("groups"),
        ),
        check_vma=False,
    )
```

```python
import functools

import jax
import jax.numpy as jnp
from jax import lax
from jax.experimental import pallas as pl
from jax.experimental.pallas import tpu as pltpu
from jax.sharding import PartitionSpec as P

GB = 2
loading = 0.05
F32 = jnp.float32
BF16 = jnp.bfloat16
MESH = pl.DeviceIdType.MESH


def split(x):
    hi = x.astype(BF16)
    return hi, (x - hi.astype(F32)).astype(BF16)


def dot(a, b):
    return jnp.dot(a, b, preferred_element_type=F32)


def dot_t(a, b):
    return lax.dot_general(a, b, (((1,), (1,)), ((), ())), preferred_element_type=F32)


def each(count, fn, first=0):
    if count - first <= 8:
        for i in range(first, count):
            fn(i)
    else:

        def step(i, c):
            fn(i)
            return c

        lax.fori_loop(first, count, step, 0)


def kernel(
    dims,
    smp, bw, sub_in, trn_in,
    cov, filt, en,
    sub, trn, sendb, recv, wfull, sel, wl, bq, wv, eacc, gat, ev, psum, esend, erecv,
    send_sem, recv_sem, fsem, rsem, lsem, near,
):
    n, cores, c_loc, gates, pulses, ns, s_n, k_half = dims
    beams = 2 * k_half
    chans = n * c_loc
    part = n // 4
    rows = part * c_loc
    core = lax.axis_index("sub")
    me = lax.axis_index("range") * cores + core
    plane, low = me // part, me % part
    upper = plane // 2
    planes = (3 - 3 * upper, 2 - upper, plane + 1 - 2 * (plane % 2), plane)

    def where(d):
        return {"range": d // cores, "sub": d % cores}

    def device(p, i):
        return planes[p] * part + (low + i) % part

    def slots(ref, g, p, count=None):
        return ref.at[g, pl.ds(planes[p] * part, count or part)]

    def fetch(d, g, p, ref):
        return pltpu.make_async_copy(smp.at[:, d * GB + g], ref.at[g, d], fsem.at[GB + min(p, 2) // 2 if p != 1 else g])

    def piece(d, g, p):
        return pltpu.make_async_remote_copy(
            src_ref=sendb.at[g, d],
            dst_ref=recv.at[g, me],
            send_sem=send_sem.at[0],
            recv_sem=recv_sem.at[g, min(p, 2) if isinstance(p, int) else p],
            device_id=where(d),
            device_id_type=MESH,
        )

    def arrived(src, dst, p, g):
        return pltpu.make_async_remote_copy(
            src_ref=src,
            dst_ref=dst,
            send_sem=send_sem.at[0],
            recv_sem=recv_sem.at[g, p],
            device_id=where(device(2, 0)),
            device_id_type=MESH,
        )

    barrier = pltpu.get_barrier_semaphore()
    below, above = (plane + 3) // 4, (6 - plane) // 4

    def greet(d):
        pl.semaphore_signal(barrier, inc=1, device_id=where(d), device_id_type=MESH)

    for there, step in ((below * above, -part), (above, part)):

        @pl.when(there == 1)
        def _():
            for j in range(cores):
                greet(me - core + step + j)

    each(part, lambda i: greet(device(3, i)), 1)

    groups = [(g, p) for p in (1, 0, 2, 3) for g in range(GB)]
    for g, p in groups:
        each(part, lambda i: fetch(device(p, i), g, p, sendb).start(), int(p == 3))
    mine = [pltpu.make_async_copy(smp.at[:, me * GB + g], recv.at[g, me], lsem.at[0]) for g in range(GB)]
    keep = pltpu.make_async_copy(bw.at[core], wfull.at[core], lsem.at[1])
    small = [
        pltpu.make_async_copy(sub_in, sub, lsem.at[2]),
        pltpu.make_async_copy(trn_in, trn, lsem.at[3]),
    ]
    for copy in mine + [keep] + small:
        copy.start()

    def ready(k):
        ref = (
            [slots(sendb, g, 1) for g in range(GB)]
            + [sendb.at[:, pl.ds(0, part)], sendb.at[:, pl.ds(0, 2 * part - 1)]]
        )[k]
        pltpu.make_async_copy(ref, ref, fsem.at[k]).wait()

    place = (plane + upper) % 2
    cell = low - core

    def send(p, i, g):
        piece(device(p, i), g, place if p < 2 else p).start()

    def send_plane(p, g):
        each(part, lambda i: send(p, i, g), int(p == 3))

    def facing(j, g):
        piece(planes[1] * part + cell + j, g, place).start()

    def others(g):
        each(part - cores, lambda i: piece(planes[1] * part + (cell + cores + i) % part, g, place).start())

    def tell(step, k):
        pl.semaphore_signal(near.at[k], inc=1, device_id=where(me + step), device_id_type=MESH)

    def hear(k):
        pl.semaphore_wait(near.at[k], 1)

    ready(0)
    pl.semaphore_wait(barrier, part - 1 + cores * (below + above * (1 - upper)))

    @pl.when(plane == 0)
    def _():
        tell(part, 2)
        for k in range(1, GB + 1):
            ready(k)
        hear(0)
        for j in range(cores):
            facing(j, 0)
        hear(1)
        others(0)
        hear(2)
        send_plane(0, 0)
        send_plane(0, 1)
        each(part // cores, lambda i: piece(planes[1] * part + part - cores * (i + 1), 1, place).start())
        for j in range(1, cores):
            each(part // cores, lambda i: piece(planes[1] * part + (cell + cores * (i + 1)) % part + j, 1, place).start())

    @pl.when(plane == 1)
    def _():
        for j in range(cores):
            facing(j, 0)
        tell(-part, 0)
        tell(part, 0)
        for k in range(1, GB + 1):
            ready(k)
        hear(0)
        tell(-part, 1)
        others(0)
        hear(2)
        tell(part, 1)
        hear(1)
        tell(-part, 2)
        send_plane(0, 0)
        send_plane(0, 1)
        each(part // cores, lambda i: piece(planes[1] * part + part - cores * (i + 1), 1, place).start())
        for j in range(1, cores):
            each(part // cores, lambda i: piece(planes[1] * part + (cell + cores * (i + 1)) % part + j, 1, place).start())

    @pl.when(plane == 2)
    def _():
        tell(-part, 0)
        for j in range(cores):
            facing(j, 0)
        for k in range(1, GB + 1):
            ready(k)
        hear(0)
        others(0)
        hear(2)
        tell(-part, 1)
        hear(1)
        tell(part, 0)
        send_plane(0, 0)
        each(part - cores, lambda i: piece(planes[0] * part + cores + (low + i) % (part - cores), 1, place).start())
        for j in range(cores):
            each(part // cores, lambda i: piece(planes[1] * part + (cell + cores * i) % part + j, 1, place).start())
        each(cores, lambda i: piece(planes[0] * part + i, 1, place).start())

    @pl.when(plane == 3)
    def _():
        tell(-part, 2)
        for k in range(1, GB + 1):
            ready(k)
        hear(0)
        send_plane(1, 0)
        send_plane(0, 0)
        each(part - cores, lambda i: piece(planes[0] * part + cores + (low + i) % (part - cores), 1, place).start())
        for j in range(cores):
            each(part // cores, lambda i: piece(planes[1] * part + (cell + cores * i) % part + j, 1, place).start())
        each(cores, lambda i: piece(planes[0] * part + i, 1, place).start())

    ready(GB + 1)
    for g, p in groups[2 * GB :]:
        send_plane(p, g)
    for copy in small:
        copy.wait()
    swap = pltpu.make_async_remote_copy(
        src_ref=bw.at[1 - core],
        dst_ref=wfull.at[core],
        send_sem=lsem.at[2],
        recv_sem=rsem.at[0],
        device_id={"sub": 1 - core},
        device_id_type=MESH,
    )
    swap.start()

    chosen = jnp.concatenate([sub[s : s + 1, :] for s in range(ns)], axis=1)
    picks = []
    for q in range(4):
        r = lax.broadcasted_iota(jnp.int32, (rows, chans), 0)
        if c_loc % 8 == 0:
            chan = r + q * rows
        else:
            chan = (q * part + r % part) * c_loc + r // part
        pick = jnp.where(chan == chosen, 1.0, 0.0).astype(F32)
        sel[q] = jnp.transpose(pick).astype(BF16)
        picks.append(pick.astype(BF16))
    keep.wait()
    swap.wait()
    sides = []
    for iq in range(2):
        cols = []
        for s in range(ns):
            cols.append(jnp.concatenate([jnp.transpose(wfull[h, s, iq]) for h in range(2)], axis=0))
        sides.append(jnp.concatenate(cols, axis=1))
    for s in range(ns):
        w_r, w_i = (jnp.concatenate([wfull[h, s, iq] for h in range(2)], axis=1) for iq in range(2))
        both = jnp.concatenate([w_r, w_i], axis=1)
        wv[s] = both
        hi, lo = split(jnp.concatenate([both, jnp.concatenate([-w_i, w_r], axis=1)], axis=0))
        bq[s, 0] = hi
        bq[s, 1] = lo
    w_hi, w_lo = split(jnp.concatenate(sides, axis=0))
    for q in range(4):
        wl[q, 0] = dot_t(w_hi, picks[q]).astype(BF16)
        wl[q, 1] = dot_t(w_lo, picks[q]).astype(BF16)

    def build(p, g):
        q = planes[p]
        sides = []
        for iq in range(2):
            j = iq * c_loc
            if c_loc % 8 == 0:
                block = recv[g, pl.ds(q * part, part), j : j + c_loc, :].reshape(rows, pulses)
            else:
                block = jnp.concatenate(
                    [
                        recv[g, pl.ds(q * part, part), j + c : j + c + 1, :].reshape(part, pulses)
                        for c in range(c_loc)
                    ],
                    axis=0,
                )
            sides.append(block)
        return split(jnp.concatenate(sides, axis=1))

    def beam(p, z_hi, z_lo):
        l_hi, l_lo = wl[planes[p], 0], wl[planes[p], 1]
        both = dot(jnp.concatenate([l_hi, l_lo], axis=1), jnp.concatenate([z_hi, z_hi], axis=0))
        return both + dot(l_hi, z_lo)

    def gather(p, z):
        picked = sel[planes[p]]
        for i in range(2):
            gat[i] = (gat[i].astype(F32) + dot(picked, z[i])).astype(BF16)

    def report(d):
        return pltpu.make_async_remote_copy(
            src_ref=esend,
            dst_ref=erecv.at[me],
            send_sem=lsem.at[3],
            recv_sem=rsem.at[1],
            device_id=where(d),
            device_id_type=MESH,
        )

    def wait_for(g, p):
        if p == 2 and g == 0:
            pltpu.make_async_copy(recv.at[:, me], recv.at[:, me], lsem.at[0]).wait()
        ref = recv.at[g, pl.ds(0, 2 * part - 1)] if p == 2 else slots(recv, g, p)
        arrived(ref, ref, p, g).wait_recv()

    factor = 1.0 / (GB * pulses)
    for g in range(GB):
        wait_for(g, 2)
        own, next_to = build(3, g), build(2, g)
        eacc[...] = beam(3, *own) + beam(2, *next_to)
        picked = jnp.concatenate([sel[planes[3]], sel[planes[2]]], axis=1)
        for i in range(2):
            gat[i] = dot(picked, jnp.concatenate([own[i], next_to[i]], axis=0)).astype(BF16)
        wait_for(g, 0)
        z = build(0, g)
        eacc[...] = eacc[...] + beam(0, *z)
        gather(0, z)
        wait_for(g, 1)
        z = build(1, g)
        full = eacc[...] + beam(1, *z)
        e_re = full[:beams, :pulses] + full[beams:, pulses:]
        e_im = full[:beams, pulses:] - full[beams:, :pulses]
        power = e_re * e_re + e_im * e_im
        if g < GB - 1:
            psum[...] = power if g == 0 else psum[...] + power
        else:
            across = jnp.transpose(psum[...] + power)
            esum = jnp.sum(across.reshape(pulses // 8, 8, beams), axis=0)
            esend[...] = esum
            erecv[me] = esum
            for j in range(3):
                other = j + (j + 4 - plane) // 4
                each(part, lambda i: report(other * part + (low + i) % part).start())
            each(part, lambda i: report(device(3, i)).start(), 1)
        ev[g, 0] = e_re
        ev[g, 1] = e_im
        gather(1, z)
        weight = trn[g].astype(F32) * factor
        for s in range(ns):
            x = [gat[i, s * s_n : (s + 1) * s_n, :] for i in range(2)]
            right = [
                jnp.concatenate([v, jnp.concatenate([-v[:, pulses:], v[:, :pulses]], axis=1)], axis=0)
                for v in x
            ]
            r_s = (dot_t(x[0], right[0]) + (dot_t(x[0], right[1]) + dot_t(x[1], right[0]))) * weight
            cov[s] = r_s if g == 0 else cov[s] + r_s
    total = jnp.zeros((8, 2 * beams), F32)
    for s in range(ns):
        r_hi, r_lo = split(cov[s])
        b_hi, b_lo = bq[s, 0], bq[s, 1]
        term = (dot(r_hi, b_hi) + (dot(r_lo, b_hi) + dot(r_hi, b_lo))) * wv[s]
        total = total + jnp.sum(term.reshape(s_n // 8, 8, 2 * beams), axis=0)
    quadratic = jnp.sum(total, axis=0, keepdims=True)
    quadratic = quadratic[:, :beams] + quadratic[:, beams:]
    inverse = 1.0 / jnp.sqrt(quadratic + loading)
    scale = jnp.transpose(jnp.broadcast_to(inverse, (pulses, beams)))
    for g in range(GB):
        for iq in range(2):
            filt[iq, pl.ds(g, beams, stride=GB), :] = ev[g, iq] * scale

    sent = sendb.at[:, pl.ds(0, n - 1)]
    pltpu.make_async_remote_copy(
        src_ref=sent,
        dst_ref=sent,
        send_sem=send_sem.at[0],
        recv_sem=recv_sem.at[0, 0],
        device_id=where(device(2, 0)),
        device_id_type=MESH,
    ).wait_send()
    reports = erecv.at[pl.ds(0, n - 1)]
    shared = pltpu.make_async_remote_copy(
        src_ref=reports,
        dst_ref=reports,
        send_sem=lsem.at[3],
        recv_sem=rsem.at[1],
        device_id=where(device(2, 0)),
        device_id_type=MESH,
    )
    shared.wait_send()
    shared.wait_recv()
    en[...] = jnp.sum(jnp.sum(erecv[...], axis=0), axis=0, keepdims=True) * (1.0 / (gates * pulses))


def store(cov, filt, en, cov_out, filt_out, en_out, sem):
    pairs = ((cov, cov_out), (filt, filt_out), (en, en_out))
    copies = [pltpu.make_async_copy(a, b, sem.at[i]) for i, (a, b) in enumerate(pairs)]
    for copy in copies:
        copy.start()
    for copy in copies:
        copy.wait()


def body(samples, beam_weights, subarrays, training):
    range_count = lax.axis_size("range")
    cores = lax.axis_size("sub")
    n = range_count * cores
    parts_iq, c_loc, gates, pulses = samples.shape
    blocks, ns, _, s_n, k_half = beam_weights.shape
    assert gates == GB * n and blocks == cores == 2 and subarrays.shape[0] == 1
    assert n & (n - 1) == 0 and n >= 8
    assert parts_iq == 2 and n * c_loc == ns * s_n
    beams, chans = 2 * k_half, n * c_loc
    dims = (n, cores, c_loc, gates, pulses, ns, s_n, k_half)
    hbm = pl.BlockSpec(memory_space=pl.ANY)
    vmem = pl.BlockSpec(memory_space=pltpu.VMEM)
    dma = pltpu.SemaphoreType.DMA
    cov, filt, en = pl.pallas_call(
        functools.partial(kernel, dims),
        out_shape=(
            pltpu.VMEM((ns, s_n, 2 * s_n), F32),
            pltpu.VMEM((2, beams * GB, pulses), F32),
            pltpu.VMEM((1, beams), F32),
        ),
        in_specs=[hbm] * 4,
        out_specs=(vmem, vmem, vmem),
        scratch_shapes=[
            pltpu.VMEM((ns, s_n), jnp.int32),
            pltpu.SMEM((GB,), jnp.int32),
            pltpu.VMEM((GB, n, 2 * c_loc, pulses), F32),
            pltpu.VMEM((GB, n, 2 * c_loc, pulses), F32),
            pltpu.VMEM((2, ns, 2, s_n, k_half), F32),
            pltpu.VMEM((4, chans, chans // 4), BF16),
            pltpu.VMEM((4, 2, 2 * beams, chans // 4), BF16),
            pltpu.VMEM((ns, 2, 2 * s_n, 2 * beams), BF16),
            pltpu.VMEM((ns, s_n, 2 * beams), F32),
            pltpu.VMEM((2 * beams, 2 * pulses), F32),
            pltpu.VMEM((2, chans, 2 * pulses), BF16),
            pltpu.VMEM((GB, 2, beams, pulses), F32),
            pltpu.VMEM((beams, pulses), F32),
            pltpu.VMEM((8, beams), F32),
            pltpu.VMEM((n, 8, beams), F32),
            dma((1,)),
            dma((GB, 3)),
            dma((GB + 2,)),
            dma((2,)),
            dma((4,)),
            pltpu.SemaphoreType.REGULAR((3,)),
        ],
        compiler_params=pltpu.CompilerParams(collective_id=0, has_side_effects=True),
    )(
        samples.reshape(2 * c_loc, gates, pulses),
        beam_weights,
        subarrays.reshape(ns, s_n),
        training,
    )
    cov, filt, en = (pltpu.with_memory_space_constraint(v, pltpu.VMEM) for v in (cov, filt, en))
    cov, filt, en = pl.pallas_call(
        store,
        out_shape=[jax.ShapeDtypeStruct(v.shape, F32) for v in (cov, filt, en)],
        in_specs=[vmem] * 3,
        out_specs=[hbm] * 3,
        scratch_shapes=[dma((3,))],
    )(cov, filt, en)
    return (
        cov.reshape(1, ns, s_n, 2 * s_n),
        filt.reshape(2, beams, GB, pulses),
        en.reshape(beams),
    )


def solution(mesh):
    placed = (
        P(None, ("groups", "range", "sub"), None, None),
        P(("groups", "range"), None, None, None, "sub"),
        P(("groups", "range", "sub"), None, None),
        P(("groups", "range", "sub")),
    )
    return jax.shard_map(
        body,
        mesh=mesh,
        in_specs=placed,
        out_specs=(
            P(("groups", "range", "sub"), None, None, None),
            P(None, None, ("groups", "range", "sub"), None),
            P("groups"),
        ),
        check_vma=False,
    )
```
